32 devices in a mesh: row: 8 (over z, core), col: 4 (over y, x).
Axes of the slice: x: 2, y: 2, z: 4, core: 2. Of those that a mesh axis runs over, the one named last changes fastest.
Arguments:
- velocity: float32 [1, 3, 64, 64, 256], P(None, None, 'row', 'col'), may hold values from -6 to 6
- tendency: float32 [1, 3, 64, 64, 256], P(None, None, 'row', 'col'), may hold values from -6 to 6
- step_size: float32 [1], replicated, may hold values from 0.1 to 0.6
- lift_weight: float32 [32, 3], replicated, may hold values from -3.5 to 3.5
- lift_bias: float32 [32], replicated, may hold values from -3 to 3
- spectral_weight: bfloat16 [2, 32, 32, 32, 1024], P(None, 'row', 'col'), may hold values from -6 to 6
- local_weight: float32 [32, 32], replicated, may hold values from -1 to 1
- local_bias: float32 [32], replicated, may hold values from -3 to 3
Outputs:
- features: bfloat16 [1, 32, 64, 64, 256], P(None, None, 'row', 'col')
The draws below stay inside these ranges and needn't reach their ends.
All inputs are finite; a program needn't handle non-finite values.
Results may differ from the reference program's by a relative error of at most 0.001.
Values sent between devices are 32-bit elements; how exact they have to be, the bound alone decides.
A program may use at most 64 MiB of HBM per device.

```python
import math
import jax
import jax.numpy as jnp
from jax import lax

CHANNELS = 32
KX = 32
KY = 32
KZ = 32
NZ = 256
SAMPLES = 1
NX = 64
NY = 64


def block_levels(key, dims, shards, low, high):
    factor_of, own = 1.0, jax.random.fold_in(key, 6)
    for position, shards_of in shards:
        heights = jnp.exp(jax.random.uniform(jax.random.fold_in(own, position), (shards_of,), jnp.float32, low / len(shards), high / len(shards)))
        factor_of = factor_of * jnp.repeat(heights, dims[position] // shards_of).reshape([-1 if axis == position else 1 for axis in range(len(dims))])
    return factor_of


def centred(key, dims, scale, reach, pieces=(), kind=jnp.bfloat16):
    gain = block_levels(key, dims, pieces, -0.22, 0.18) if pieces else 1.0
    entries = jax.random.normal(key, dims, jnp.float32) * scale * gain
    return jnp.minimum(jnp.maximum(entries, -reach), reach).astype(kind)


def setup_inputs(seed: int = 0) -> dict:
    arg_keys = jax.random.split(jax.random.key(seed), 9)
    velocity = centred(arg_keys[0], (SAMPLES, 3, NX, NY, NZ), 1.0, 6.0, ((2, 8), (3, 4)), jnp.float32)
    tendency = centred(arg_keys[1], (SAMPLES, 3, NX, NY, NZ), 1.0, 6.0, ((2, 8), (3, 4)), jnp.float32)
    step_size = jnp.clip(jnp.exp(jax.random.uniform(arg_keys[2], (SAMPLES,), jnp.float32, math.log(0.1), math.log(0.6))), 0.1, 0.6)
    lift_weight = centred(arg_keys[3], (CHANNELS, 3), 3 ** -0.5, 3.5, (), jnp.float32)
    lift_bias = centred(arg_keys[4], (CHANNELS,), 0.5, 3.0, (), jnp.float32)
    spectral_weight = centred(arg_keys[5], (2, KY, KZ, KX, CHANNELS * CHANNELS), 1.0, 6.0, ((1, 8), (2, 4)))
    local_weight = centred(arg_keys[6], (CHANNELS, CHANNELS), CHANNELS ** -0.5, 1.0, (), jnp.float32)
    local_bias = centred(arg_keys[7], (CHANNELS,), 0.5, 3.0, (), jnp.float32)
    return dict(velocity=velocity, tendency=tendency, step_size=step_size, lift_weight=lift_weight, lift_bias=lift_bias, spectral_weight=spectral_weight, local_weight=local_weight, local_bias=local_bias)


def positions(count, length):
    index = jnp.arange(count, dtype=jnp.int32)
    return jnp.where(index < count // 2, index, length - count + index).astype(jnp.int32)


def reference(velocity, tendency, step_size, lift_weight, lift_bias, spectral_weight, local_weight, local_bias):
    highest = lax.Precision.HIGHEST
    x_pos = positions(KX, NX)
    y_pos = positions(KY, NY)
    z_pos = jnp.arange(KZ, dtype=jnp.int32)
    volume = NX * NY * NZ
    weights = spectral_weight.astype(jnp.float32).reshape(2, KY, KZ, KX, CHANNELS, CHANNELS)
    complex_weights = weights[0] + 1j * weights[1]
    combined = jnp.dot(local_weight, lift_weight, precision=highest)
    offset = jnp.dot(local_weight, lift_bias, precision=highest) + local_bias
    results = []
    for sample in range(SAMPLES):
        advanced = velocity[sample] + step_size[sample] * tendency[sample]

        def forward(channel):
            lifted = (lift_weight[channel, 0] * advanced[0] + lift_weight[channel, 1] * advanced[1]
                      + lift_weight[channel, 2] * advanced[2] + lift_bias[channel])
            spectrum = jnp.fft.rfftn(lifted)
            kept = spectrum[x_pos][:, y_pos][:, :, :KZ]
            return kept / volume

        coeffs = lax.map(forward, jnp.arange(CHANNELS, dtype=jnp.int32))
        mixed = jnp.einsum("egaoi,iaeg->oaeg", complex_weights, coeffs, precision=highest)

        def inverse(channel):
            full = jnp.zeros((NX, NY, NZ // 2 + 1), mixed.dtype)
            full = full.at[x_pos[:, None, None], y_pos[None, :, None], z_pos[None, None, :]].set(mixed[channel])
            spectral = jnp.fft.irfftn(full, s=(NX, NY, NZ)) * volume
            local = (combined[channel, 0] * advanced[0] + combined[channel, 1] * advanced[1]
                     + combined[channel, 2] * advanced[2] + offset[channel])
            return jax.nn.gelu(spectral + local).astype(jnp.bfloat16)

        results.append(lax.map(inverse, jnp.arange(CHANNELS, dtype=jnp.int32)))
    return jnp.stack(results, 0)
```

```python
import functools
import math

import jax
import jax.numpy as jnp
import numpy as np
from jax import lax
from jax.experimental import pallas as pl
from jax.experimental.pallas import tpu as pltpu
from jax.sharding import PartitionSpec as P

KX = 32
KY = 32
KZ = 32
LANES = 128
HIGHEST = lax.Precision.HIGHEST
F32 = jnp.float32
BF16 = jnp.bfloat16
MESH = pl.DeviceIdType.MESH


def waves(count):
    index = np.arange(count)
    return np.where(index < count // 2, index, index - count)


def trig(wave, length):
    angle = ((wave[:, None] * np.arange(length)[None, :]) % length) * (2.0 * math.pi / length)
    return np.cos(angle), np.sin(angle)


def np_halves(table):
    table = np.asarray(table, np.float32)
    high = table.astype(jnp.bfloat16)
    low = (table - high.astype(np.float32)).astype(jnp.bfloat16)
    return high, low


def split(x):
    high = x.astype(BF16)
    return high, (x - high.astype(F32)).astype(BF16)


def stacked(x):
    high = x.astype(BF16).astype(F32)
    return jnp.concatenate([high, x - high], 0).astype(BF16)


def dot(a, b):
    return jnp.dot(a, b, preferred_element_type=F32)


def dot_rows(a, b, precision=None):
    return lax.dot_general(a, b, (((0,), (0,)), ((), ())), precision=precision, preferred_element_type=F32)


def dot_lanes(a, b):
    return lax.dot_general(a, b, (((1,), (1,)), ((), ())), preferred_element_type=F32)


def iota(shape, axis):
    return lax.broadcasted_iota(jnp.int32, shape, axis)


def one_channel(d, row, adv_ref, tz):
    width_in = adv_ref.shape[0]
    d = d + jnp.where(iota(d.shape, 0) == 0, row(width_in), 0.0)
    high, low = split(d)
    x = dot_rows(jnp.concatenate([high, low, high], 0), tz)
    for j in range(width_in):
        weight = row(j)
        x = x + jnp.concatenate([weight] * (x.shape[1] // LANES), 1) * adv_ref[j]
    inner = x * (0.7978845608028654 + 0.035677408136300125 * (x * x))
    half = 0.5 * x
    return (half + half * jnp.tanh(inner)).astype(BF16)


def layer_kernel(
    kyl, kzl, oc, lag, vel_any, tend_any, step_any, lw_any, lb_any, cw_any, cb_any, zf_any, yfh_any, yfl_any, xf_any,
    sel_any, xb_any, yh_any, yl_any, tz_any, w_any, *rest,
):
    chunks = LANES // (oc * (lw_any.shape[0] + 1))
    if chunks > 1:
        feats_ref, rest = rest[0], rest[1:]
    else:
        feats_ref = None
    (
        dlast_ref, adv_ref, comb_ref, vel_ref, tend_ref, step_ref, lw_ref, lb_ref, cw_ref, cb_ref, zf_ref, yfh_ref,
        yfl_ref, xf_ref, sel_ref, xb_ref, yh_ref, yl_ref, tz_ref, w_ref, lift_ref, wl_ref, wt_ref, yexp_ref, zsend, zrecv,
        ypad, ysend, yrecv, amp_ref, xsend, xrecv, csend, crecv, in_sems, z_ss, z_rs, y_ss, y_rs, x_ss, x_rs, c_ss, c_rs,
    ) = rest
    rows, cols = lax.axis_size("row"), lax.axis_size("col")
    my_row, my_col = lax.axis_index("row"), lax.axis_index("col")
    width_in, cells, _ = vel_ref.shape
    channels = cw_ref.shape[0]
    group = width_in + 1
    freq = zf_ref.shape[0] // 2
    rk = freq // cols
    slots = kyl * kzl
    modes = slots * KX
    ko = kzl * oc

    loads = {}
    order = [
        ("vel", vel_any, vel_ref), ("tend", tend_any, tend_ref), ("step", step_any, step_ref), ("zf", zf_any, zf_ref),
        ("lw", lw_any, lw_ref), ("lb", lb_any, lb_ref), ("cw", cw_any, cw_ref), ("cb", cb_any, cb_ref),
        ("w", w_any, w_ref), ("yfh", yfh_any, yfh_ref), ("yfl", yfl_any, yfl_ref), ("yh", yh_any, yh_ref),
        ("yl", yl_any, yl_ref), ("xf", xf_any, xf_ref), ("sel", sel_any, sel_ref), ("xb", xb_any, xb_ref),
        ("tz", tz_any, tz_ref),
    ]
    for n, (name, source, target) in enumerate(order):
        loads[name] = pltpu.make_async_copy(source, target, in_sems.at[n])
        loads[name].start()

    def loaded(*names):
        for name in names:
            loads[name].wait()

    barrier = pltpu.get_barrier_semaphore()
    row_peers = [lax.rem(my_row + i, rows) for i in range(1, rows)]
    col_peers = [lax.rem(my_col + i, cols) for i in range(1, cols)]
    for peer in row_peers:
        pl.semaphore_signal(barrier, inc=1, device_id={"row": peer}, device_id_type=MESH)
    for peer in col_peers:
        pl.semaphore_signal(barrier, inc=1, device_id={"col": peer}, device_id_type=MESH)

    def send(source, target, sends, receives, **where):
        copy = pltpu.make_async_remote_copy(source, target, sends, receives, device_id=where, device_id_type=MESH)
        copy.start()
        return copy

    loaded("vel", "tend", "step", "zf")
    step = step_ref[0:1, 0:1]
    for j in range(width_in):
        adv = vel_ref[j] + step * tend_ref[j]
        adv_ref[j] = adv
        high, low = split(adv)
        both = dot_lanes(zf_ref[...], high)
        z = both[:freq] + both[freq:] + dot_lanes(zf_ref[0:freq, :], low)
        zsend[:, j * rk:(j + 1) * rk, :] = z.reshape(cols, rk, cells)
    pl.semaphore_wait(barrier, rows + cols - 2)
    z_copies = [
        send(zsend.at[peer], zrecv.at[my_col], z_ss.at[i], z_rs.at[i], col=peer) for i, peer in enumerate(col_peers)
    ]
    zrecv[pl.ds(my_col, 1)] = zsend[pl.ds(my_col, 1)]

    loaded("lw", "lb", "cw", "cb")
    eight = iota((8, channels), 0)
    lift = jnp.where(eight == width_in, lb_ref[...], 0.0)
    for j in range(width_in):
        lift = jnp.where(eight == j, lw_ref[j:j + 1, :], lift)
    block = iota((8, LANES), 1) // oc
    pick = jnp.where(block % group == iota((8, LANES), 0), 1.0, 0.0)
    spread = dot_rows(lift, pick, HIGHEST)
    high = spread.astype(BF16).astype(F32)
    low = spread - high
    lane = iota((channels, LANES), 1)
    owner = (lane // (oc * group)) * oc + lane % oc
    for o in range(channels):
        at = slice(o * channels, (o + 1) * channels)
        lift_ref[at, :LANES] = jnp.where(owner == o, high, 0.0).astype(BF16)
        lift_ref[at, LANES:] = jnp.where(owner == o, low, 0.0).astype(BF16)
    wide = (8, group * LANES)
    spread = dot_rows(lift, jnp.where(iota(wide, 1) // LANES == iota(wide, 0), 1.0, 0.0), HIGHEST)
    comb = jnp.dot(cw_ref[...], spread, precision=HIGHEST, preferred_element_type=F32)
    bias = jnp.where(eight == 0, cb_ref[...], 0.0)
    bias = dot_rows(bias, jnp.where(iota((8, LANES), 0) == 0, 1.0, 0.0), HIGHEST)
    comb_ref[:, :width_in * LANES] = comb[:, :width_in * LANES]
    comb_ref[:, width_in * LANES:] = comb[:, width_in * LANES:] + bias

    loaded("w")
    step_rows = modes // 2

    def weigh(n):
        at = slice(n * step_rows, (n + 1) * step_rows)
        both = dot(w_ref[at, :], lift_ref[...])
        wl_ref[at, :] = both[:, :LANES] + both[:, LANES:]

    weigh(0)
    weigh(1)
    loaded("yfh", "yfl")
    for copy in z_copies:
        copy.wait_recv()

    x = jnp.concatenate([zrecv[s] for s in range(cols)], 1)
    depth = width_in * rk
    halves = stacked(x)
    both = dot(halves, yfh_ref[...])
    y = both[:depth] + both[depth:] + dot(x.astype(BF16), yfl_ref[...])
    lanes = yfh_ref.shape[1] // 2
    wide = ypad.shape[1]
    parts = lanes // wide
    slot = ypad.shape[0] // parts
    ypad[...] = jnp.zeros_like(ypad)
    low_rows = iota((rk, lanes), 0) < rk // 2
    for j in range(width_in):
        here = y[j * rk:(j + 1) * rk]
        turned = pltpu.roll(here[:, lanes:], rk // 2, 0)
        here = here[:, :lanes] + jnp.where(low_rows, turned, -turned)
        for p in range(parts):
            ypad[p * slot + j * rk:p * slot + (j + 1) * rk, :] = here[:, p * wide:(p + 1) * wide]
    ysend[...] = jnp.transpose(ypad[...]).reshape(ysend.shape)
    y_copies = [
        send(ysend.at[peer], yrecv.at[my_row], y_ss.at[i], y_rs.at[i], row=peer) for i, peer in enumerate(row_peers)
    ]
    yrecv[pl.ds(my_row, 1)] = ysend[pl.ds(my_row, 1)]

    weigh(2)
    weigh(3)

    def turn(n, carry):
        ri, at = n // (KX // 8), (n % (KX // 8)) * 8
        held = [wl_ref[pl.ds(pl.multiple_of(ri * modes + s * KX + at, 8), 8), :] for s in range(slots)]
        place = iota((8, LANES), 1) // oc
        bit = 1
        while bit < slots:
            upper = (place // bit) % 2 == 1
            for s in range(slots):
                if not s & bit:
                    a, b = held[s], held[s | bit]
                    held[s] = jnp.where(upper, pltpu.roll(b, bit * oc, 1), a)
                    held[s | bit] = jnp.where(upper, b, pltpu.roll(a, LANES - bit * oc, 1))
            bit *= 2
        for s in range(slots):
            wt_ref[ri, s, pl.ds(pl.multiple_of(at, 8), 8), :] = held[s]
        return carry

    lax.fori_loop(0, 2 * (KX // 8), turn, 0)

    loaded("yh", "yl")
    pairs = 2 * rows
    a = xsend.shape[2] // 2
    total = pairs * a
    width = 2 * cells
    same = iota((pairs, a, width), 1) == (iota((pairs, a, width), 2) // (cells // a)) % a

    def expand(d, carry):
        for h, table in enumerate((yh_ref, yl_ref)):
            for l in range(kyl):
                full = jnp.where(same, table[d, l].astype(F32)[:, None, :], 0.0)
                yexp_ref[d, h, l * total:(l + 1) * total, :] = full.reshape(total, width).astype(BF16)
        return carry

    lax.fori_loop(0, cols, expand, 0)
    loaded("xf", "sel", "xb", "tz")
    for copy in y_copies:
        copy.wait_recv()

    deep = yrecv.shape[1] // a
    is_re = (iota((rows * a, LANES), 1) % rk) < rk // 2
    plain, cross = [], []
    for l in range(deep):
        u = yrecv[:, l * a:(l + 1) * a, :].reshape(rows * a, LANES)
        plain.append(u)
        cross.append(jnp.where(is_re, pltpu.roll(u, LANES - rk // 2, 1), -pltpu.roll(u, rk // 2, 1)))
    u = jnp.concatenate([jnp.concatenate(plain, 1), jnp.concatenate(cross, 1)], 0)
    high, low = split(u)
    both = dot(xf_ref[...], high)
    q = both[:KX] + both[KX:] + dot(xf_ref[0:KX, :], low)
    both = dot(stacked(q), sel_ref[...])
    amp_ref[...] = both[:KX] + both[KX:]
    origin = jnp.where((my_row == 0) & (my_col == 0), 1.0, 0.0)
    flag = jnp.where((iota((KX, LANES), 0) == 0) & (iota((KX, LANES), 1) < oc), origin, 0.0)

    x_copies = []
    for c in range(chunks):
        pr = wt_ref[0, c * group + width_in] * flag
        pi = wt_ref[1, c * group + width_in] * flag
        for j in range(width_in):
            wr, wi = wt_ref[0, c * group + j], wt_ref[1, c * group + j]
            ar = amp_ref[:, (2 * j) * LANES:(2 * j + 1) * LANES]
            ai = amp_ref[:, (2 * j + 1) * LANES:(2 * j + 2) * LANES]
            pr = pr + (wr * ar - wi * ai)
            pi = pi + (wr * ai + wi * ar)
        high, low = split(jnp.concatenate([pr, pi], 0))
        xsend[c] = dot(xb_ref[...], jnp.concatenate([high, low, high], 0)).reshape(xsend.shape[1:])
        x_copies.append([
            send(xsend.at[c, peer], xrecv.at[c, my_row], x_ss.at[c, i], x_rs.at[c, i], row=peer)
            for i, peer in enumerate(row_peers)
        ])
        xrecv[c, pl.ds(my_row, 1)] = xsend[c, pl.ds(my_row, 1)]

    tz = tz_ref[...]
    c_copies = []

    def landing(c):
        return dlast_ref if c == chunks - 1 else crecv.at[c]

    def inverse_y(c):
        for copy in x_copies[c]:
            copy.wait_recv()
        turned = jnp.transpose(xrecv[c].reshape(total, LANES))
        held = jnp.concatenate([turned[l * ko:(l + 1) * ko] for l in range(kyl)], 1)
        halves = stacked(held)
        at = pl.ds(pl.multiple_of(my_col * 2 * ko, 2 * ko), 2 * ko)
        started = []
        for i in list(range(1, cols)) + [0]:
            d = lax.rem(my_col + i, cols)
            both = dot(halves, yexp_ref[d, 0])
            acc = both[:ko] + both[ko:] + dot(halves[:ko], yexp_ref[d, 1])
            acc = jnp.concatenate([acc[:, v * cells:(v + 1) * cells] for v in range(2)], 0)
            if i == 0:
                landing(c)[at, :] = acc
            else:
                csend[c, i - 1] = acc
                started.append(
                    send(csend.at[c, i - 1], landing(c).at[at, :], c_ss.at[c, i - 1], c_rs.at[c, i - 1], col=d)
                )
        c_copies.append(started)

    def inverse_z(c):
        for copy in c_copies[c]:
            copy.wait_recv()
        for i in range(oc):
            o = c * oc + i
            row = lambda j: comb_ref[o:o + 1, j * LANES:(j + 1) * LANES]
            d = crecv[c, pl.ds(i, cols * 2 * kzl, stride=oc), :]
            feats_ref[o] = one_channel(d, row, adv_ref, tz)

    for c in range(chunks):
        inverse_y(c)
        if 0 <= c - lag < chunks - 1:
            inverse_z(c - lag)
    for c in range(max(chunks - lag, 0), chunks - 1):
        inverse_z(c)
    for copy in c_copies[chunks - 1]:
        copy.wait_recv()
    for copies in [z_copies, y_copies] + x_copies + c_copies:
        for copy in copies:
            copy.wait_send()


def finish_kernel(oc, depth, *refs):
    if len(refs) == 8:
        feats_ref, refs = refs[0], refs[1:]
        first = feats_ref.shape[0]
    else:
        feats_ref, first = None, 0
    d_ref, adv_ref, comb_ref, tz_ref, out_ref, last_ref, sems = refs
    copies = []
    if feats_ref is not None:
        copies.append(pltpu.make_async_copy(feats_ref, out_ref.at[pl.ds(0, first)], sems.at[oc]))
        copies[0].start()
    for i in range(oc):
        o = first + i
        row = lambda j: comb_ref[o:o + 1, j * LANES:(j + 1) * LANES]
        last_ref[i] = one_channel(d_ref[pl.ds(i, depth, stride=oc), :], row, adv_ref, tz_ref[...])
        copy = pltpu.make_async_copy(last_ref.at[pl.ds(i, 1)], out_ref.at[pl.ds(o, 1)], sems.at[i])
        copy.start()
        copies.append(copy)
    for copy in copies:
        copy.wait()


def per_device(
    velocity, tendency, step_size, lift_weight, lift_bias, spectral_weight, local_weight, local_bias
):
    samples, width_in, a, b, nz = velocity.shape
    channels = lift_weight.shape[0]
    rows, cols = lax.axis_size("row"), lax.axis_size("col")
    full_x, full_y = a * rows, b * cols
    kzl, kyl = KZ // cols, KY // rows
    slots = kyl * kzl
    modes = slots * KX
    cells = a * b
    group = width_in + 1
    oc = LANES // slots
    chunks = channels // oc
    ko = kzl * oc
    lag = 3
    vmem = pl.BlockSpec(memory_space=pltpu.VMEM)
    anywhere = pl.BlockSpec(memory_space=pl.ANY)
    stored = spectral_weight.reshape(2 * modes, channels * channels)

    zc, zs = trig(np.arange(KZ), nz)
    rk = 2 * max(kzl, 4)
    zf = np.zeros((cols, 2, rk // 2, nz), np.float32)
    zf[:, :, :kzl] = np.stack([zc, -zs], 0).reshape(2, cols, kzl, nz).transpose(1, 0, 2, 3)
    zf2 = np.concatenate(np_halves(zf.reshape(cols * rk, nz)), 0)
    yc, ys = trig(waves(KY), full_y)
    xc, xs = trig(waves(KX), full_x)
    scale = 1.0 / (full_x * full_y * nz)
    xf2 = np.concatenate(np_halves(np.concatenate([xc, xs], 1) * scale), 0)
    parts = 2
    deep = kyl // parts
    slot = LANES // parts
    yf = np.stack([yc, ys], 0).reshape(2, rows, deep, parts, 1, cols, 1, b)
    yf = yf * np.eye(a).reshape(1, 1, 1, 1, a, 1, a, 1)
    yf = yf.transpose(0, 3, 1, 2, 4, 5, 6, 7).reshape(2 * parts * rows * deep * a, cols * cells).T
    yfh, yfl = np_halves(yf)
    sel = np.zeros((deep, parts, slot, width_in, 2, kyl, kzl, oc), np.float32)
    for l in range(kyl):
        for j in range(width_in):
            for ri in range(2):
                for k in range(kzl):
                    sel[l // parts, l % parts, j * rk + ri * (rk // 2) + k, j, ri, l, k] = 1
    sel = sel.reshape(deep * LANES, width_in * 2 * LANES)
    xb = np.stack([np.stack([xc, -xs], 0), np.stack([xs, xc], 0)], 0)
    xb = xb.reshape(2, 2, KX, rows, a).transpose(3, 0, 4, 1, 2).reshape(rows * 2 * a, 2 * KX)
    xbh, xbl = np_halves(xb)
    xb3 = np.concatenate([xbh, xbh, xbl], 1)
    yb = np.stack([np.stack([yc, ys], 0), np.stack([-ys, yc], 0)], 0)
    yb = yb.reshape(2, 2, rows, kyl, cols, b).transpose(4, 3, 2, 0, 1, 5)
    yb = np.broadcast_to(yb[..., None, :], (cols, kyl, rows, 2, 2, a, b)).reshape(cols, kyl, rows * 2, 2 * cells)
    ybh, ybl = np_halves(yb)
    twice = np.where(np.arange(KZ) == 0, 1.0, 2.0)[:, None]
    zb = np.stack([twice * zc, -twice * zs], 0).reshape(2, cols, kzl, nz).transpose(1, 0, 2, 3).reshape(2 * KZ, nz)
    zbh, zbl = np_halves(zb)
    zb3 = np.concatenate([zbh, zbh, zbl], 0)
    tz = jnp.asarray(zb3)

    results = []
    for sample in range(samples):
        inputs = [
            velocity[sample].reshape(width_in, cells, nz), tendency[sample].reshape(width_in, cells, nz),
            step_size[sample].reshape(1, 1), lift_weight.T, lift_bias.reshape(1, channels), local_weight,
            local_bias.reshape(1, channels), jnp.asarray(zf2), jnp.asarray(yfh), jnp.asarray(yfl), jnp.asarray(xf2),
            jnp.asarray(sel, BF16), jnp.asarray(xb3), jnp.asarray(ybh), jnp.asarray(ybl), tz, stored,
        ]
        dma = lambda *shape: pltpu.SemaphoreType.DMA(shape)
        first = channels - oc
        outs = [
            jax.ShapeDtypeStruct((cols * 2 * ko, cells), F32),
            jax.ShapeDtypeStruct((width_in, cells, nz), F32),
            jax.ShapeDtypeStruct((channels, group * LANES), F32),
        ]
        if first:
            outs = [jax.ShapeDtypeStruct((first, cells, nz), BF16)] + outs
        held = pl.pallas_call(
            functools.partial(layer_kernel, kyl, kzl, oc, lag),
            out_shape=outs,
            in_specs=[anywhere] * len(inputs),
            out_specs=[vmem] * len(outs),
            scratch_shapes=[pltpu.VMEM(x.shape, x.dtype) for x in inputs] + [
                pltpu.VMEM((channels * channels, 2 * LANES), BF16),
                pltpu.VMEM((2 * modes, LANES), F32),
                pltpu.VMEM((2, slots, KX, LANES), F32),
                pltpu.VMEM((cols, 2, kyl * rows * 2 * a, 2 * cells), BF16),
                pltpu.VMEM((cols, width_in * rk, cells), F32),
                pltpu.VMEM((cols, width_in * rk, cells), F32),
                pltpu.VMEM((parts * slot, rows * deep * a), F32),
                pltpu.VMEM((rows, deep * a, LANES), F32),
                pltpu.VMEM((rows, deep * a, LANES), F32),
                pltpu.VMEM((KX, width_in * 2 * LANES), F32),
                pltpu.VMEM((chunks, rows, 2 * a, LANES), F32),
                pltpu.VMEM((chunks, rows, 2 * a, LANES), F32),
                pltpu.VMEM((chunks, cols - 1, 2 * ko, cells), F32),
                pltpu.VMEM((chunks, cols * 2 * ko, cells), F32),
                dma(len(inputs)),
                dma(cols - 1), dma(cols - 1), dma(rows - 1), dma(rows - 1),
                dma(chunks, rows - 1), dma(chunks, rows - 1), dma(chunks, cols - 1), dma(chunks, cols - 1),
            ],
            compiler_params=pltpu.CompilerParams(
                vmem_limit_bytes=40 * 1024 * 1024, collective_id=0, has_side_effects=True
            ),
        )(*inputs)
        features = pl.pallas_call(
            functools.partial(finish_kernel, oc, cols * 2 * kzl),
            out_shape=jax.ShapeDtypeStruct((channels, cells, nz), BF16),
            in_specs=[vmem] * (len(held) + 1),
            out_specs=anywhere,
            scratch_shapes=[pltpu.VMEM((oc, cells, nz), BF16), dma(oc + 1)],
            compiler_params=pltpu.CompilerParams(vmem_limit_bytes=16 * 1024 * 1024),
        )(*held, tz)
        results.append(features.reshape(channels, a, b, nz))
    return jnp.stack(results, 0)


def solution(mesh):
    in_specs = (
        P(None, None, "row", "col", None),
        P(None, None, "row", "col", None),
        P(),
        P(),
        P(),
        P(None, "row", "col", None, None),
        P(),
        P(),
    )
    out_specs = P(None, None, "row", "col", None)
    return jax.shard_map(
        per_device, mesh=mesh, in_specs=in_specs, out_specs=out_specs, check_vma=False
    )
```

```python
import functools
import math

import jax
import jax.numpy as jnp
import numpy as np
from jax import lax
from jax.experimental import pallas as pl
from jax.experimental.pallas import tpu as pltpu
from jax.sharding import PartitionSpec as P

KX = 32
KY = 32
KZ = 32
LANES = 128
HIGHEST = lax.Precision.HIGHEST
F32 = jnp.float32
BF16 = jnp.bfloat16
MESH = pl.DeviceIdType.MESH


def waves(count):
    index = np.arange(count)
    return np.where(index < count // 2, index, index - count)


def trig(wave, length):
    angle = ((wave[:, None] * np.arange(length)[None, :]) % length) * (2.0 * math.pi / length)
    return np.cos(angle), np.sin(angle)


def np_halves(table):
    table = np.asarray(table, np.float32)
    high = table.astype(jnp.bfloat16)
    low = (table - high.astype(np.float32)).astype(jnp.bfloat16)
    return high, low


def split(x):
    high = x.astype(BF16)
    return high, (x - high.astype(F32)).astype(BF16)


def stacked(x):
    high = x.astype(BF16).astype(F32)
    return jnp.concatenate([high, x - high], 0).astype(BF16)


def dot(a, b):
    return jnp.dot(a, b, preferred_element_type=F32)


def dot_rows(a, b, precision=None):
    return lax.dot_general(a, b, (((0,), (0,)), ((), ())), precision=precision, preferred_element_type=F32)


def dot_lanes(a, b):
    return lax.dot_general(a, b, (((1,), (1,)), ((), ())), preferred_element_type=F32)


def iota(shape, axis):
    return lax.broadcasted_iota(jnp.int32, shape, axis)


def one_channel(d, row, adv_ref, tz):
    width_in = adv_ref.shape[0]
    d = d + jnp.where(iota(d.shape, 0) == 0, row(width_in), 0.0)
    high, low = split(d)
    x = dot_rows(jnp.concatenate([high, low, high], 0), tz)
    for j in range(width_in):
        weight = row(j)
        x = x + jnp.concatenate([weight] * (x.shape[1] // LANES), 1) * adv_ref[j]
    inner = x * (0.7978845608028654 + 0.035677408136300125 * (x * x))
    half = 0.5 * x
    return (half + half * jnp.tanh(inner)).astype(BF16)


def layer_kernel(
    kyl, kzl, oc, lag, vel_any, tend_any, step_any, lw_any, lb_any, cw_any, cb_any, zf_any, yfh_any, yfl_any, xf_any,
    sel_any, xb_any, yh_any, yl_any, tz_any, w_any, *rest,
):
    chunks = LANES // (oc * (lw_any.shape[0] + 1))
    if chunks > 1:
        feats_ref, rest = rest[0], rest[1:]
    else:
        feats_ref = None
    (
        dlast_ref, adv_ref, comb_ref, vel_ref, tend_ref, step_ref, lw_ref, lb_ref, cw_ref, cb_ref, zf_ref, yfh_ref,
        yfl_ref, xf_ref, sel_ref, xb_ref, yh_ref, yl_ref, tz_ref, w_ref, lift_ref, wl_ref, wt_ref, yexp_ref, zsend, zrecv,
        ypad, ysend, yrecv, amp_ref, xsend, xrecv, csend, crecv, in_sems, z_ss, z_rs, y_ss, y_rs, x_ss, x_rs, c_ss, c_rs,
    ) = rest
    rows, cols = lax.axis_size("row"), lax.axis_size("col")
    my_row, my_col = lax.axis_index("row"), lax.axis_index("col")
    width_in, cells, _ = vel_ref.shape
    channels = cw_ref.shape[0]
    group = width_in + 1
    freq = zf_ref.shape[0] // 2
    rk = freq // cols
    slots = kyl * kzl
    modes = slots * KX
    ko = kzl * oc

    loads = {}
    order = [
        ("vel", vel_any, vel_ref), ("tend", tend_any, tend_ref), ("step", step_any, step_ref), ("zf", zf_any, zf_ref),
        ("lw", lw_any, lw_ref), ("lb", lb_any, lb_ref), ("cw", cw_any, cw_ref), ("cb", cb_any, cb_ref),
        ("w", w_any, w_ref), ("yfh", yfh_any, yfh_ref), ("yfl", yfl_any, yfl_ref), ("yh", yh_any, yh_ref),
        ("yl", yl_any, yl_ref), ("xf", xf_any, xf_ref), ("sel", sel_any, sel_ref), ("xb", xb_any, xb_ref),
        ("tz", tz_any, tz_ref),
    ]
    for n, (name, source, target) in enumerate(order):
        loads[name] = pltpu.make_async_copy(source, target, in_sems.at[n])
        loads[name].start()

    def loaded(*names):
        for name in names:
            loads[name].wait()

    barrier = pltpu.get_barrier_semaphore()
    row_peers = [lax.rem(my_row + i, rows) for i in range(1, rows)]
    col_peers = [lax.rem(my_col + i, cols) for i in range(1, cols)]
    for peer in row_peers:
        pl.semaphore_signal(barrier, inc=1, device_id={"row": peer}, device_id_type=MESH)
    for peer in col_peers:
        pl.semaphore_signal(barrier, inc=1, device_id={"col": peer}, device_id_type=MESH)

    def send(source, target, sends, receives, **where):
        copy = pltpu.make_async_remote_copy(source, target, sends, receives, device_id=where, device_id_type=MESH)
        copy.start()
        return copy

    loaded("vel", "tend", "step", "zf")
    step = step_ref[0:1, 0:1]
    for j in range(width_in):
        adv = vel_ref[j] + step * tend_ref[j]
        adv_ref[j] = adv
        high, low = split(adv)
        both = dot_lanes(zf_ref[...], high)
        z = both[:freq] + both[freq:] + dot_lanes(zf_ref[0:freq, :], low)
        zsend[:, j * rk:(j + 1) * rk, :] = z.reshape(cols, rk, cells)
    pl.semaphore_wait(barrier, rows + cols - 2)
    z_copies = [
        send(zsend.at[peer], zrecv.at[my_col], z_ss.at[i], z_rs.at[i], col=peer) for i, peer in enumerate(col_peers)
    ]
    zrecv[pl.ds(my_col, 1)] = zsend[pl.ds(my_col, 1)]

    loaded("lw", "lb", "cw", "cb")
    eight = iota((8, channels), 0)
    lift = jnp.where(eight == width_in, lb_ref[...], 0.0)
    for j in range(width_in):
        lift = jnp.where(eight == j, lw_ref[j:j + 1, :], lift)
    block = iota((8, LANES), 1) // oc
    pick = jnp.where(block % group == iota((8, LANES), 0), 1.0, 0.0)
    spread = dot_rows(lift, pick, HIGHEST)
    high = spread.astype(BF16).astype(F32)
    low = spread - high
    lane = iota((channels, LANES), 1)
    owner = (lane // (oc * group)) * oc + lane % oc
    for o in range(channels):
        at = slice(o * channels, (o + 1) * channels)
        lift_ref[at, :LANES] = jnp.where(owner == o, high, 0.0).astype(BF16)
        lift_ref[at, LANES:] = jnp.where(owner == o, low, 0.0).astype(BF16)
    wide = (8, group * LANES)
    spread = dot_rows(lift, jnp.where(iota(wide, 1) // LANES == iota(wide, 0), 1.0, 0.0), HIGHEST)
    comb = jnp.dot(cw_ref[...], spread, precision=HIGHEST, preferred_element_type=F32)
    bias = jnp.where(eight == 0, cb_ref[...], 0.0)
    bias = dot_rows(bias, jnp.where(iota((8, LANES), 0) == 0, 1.0, 0.0), HIGHEST)
    comb_ref[:, :width_in * LANES] = comb[:, :width_in * LANES]
    comb_ref[:, width_in * LANES:] = comb[:, width_in * LANES:] + bias

    loaded("w")
    step_rows = modes // 2

    def weigh(n):
        at = slice(n * step_rows, (n + 1) * step_rows)
        both = dot(w_ref[at, :], lift_ref[...])
        wl_ref[at, :] = both[:, :LANES] + both[:, LANES:]

    weigh(0)
    weigh(1)
    loaded("yfh", "yfl")
    for copy in z_copies:
        copy.wait_recv()

    x = jnp.concatenate([zrecv[s] for s in range(cols)], 1)
    depth = width_in * rk
    halves = stacked(x)
    both = dot(halves, yfh_ref[...])
    y = both[:depth] + both[depth:] + dot(x.astype(BF16), yfl_ref[...])
    lanes = yfh_ref.shape[1] // 2
    wide = ypad.shape[1]
    parts = lanes // wide
    slot = ypad.shape[0] // parts
    ypad[...] = jnp.zeros_like(ypad)
    low_rows = iota((rk, lanes), 0) < rk // 2
    for j in range(width_in):
        here = y[j * rk:(j + 1) * rk]
        turned = pltpu.roll(here[:, lanes:], rk // 2, 0)
        here = here[:, :lanes] + jnp.where(low_rows, turned, -turned)
        for p in range(parts):
            ypad[p * slot + j * rk:p * slot + (j + 1) * rk, :] = here[:, p * wide:(p + 1) * wide]
    ysend[...] = jnp.transpose(ypad[...]).reshape(ysend.shape)
    y_copies = [
        send(ysend.at[peer], yrecv.at[my_row], y_ss.at[i], y_rs.at[i], row=peer) for i, peer in enumerate(row_peers)
    ]
    yrecv[pl.ds(my_row, 1)] = ysend[pl.ds(my_row, 1)]

    weigh(2)
    weigh(3)

    def turn(n, carry):
        ri, at = n // (KX // 8), (n % (KX // 8)) * 8
        held = [wl_ref[pl.ds(pl.multiple_of(ri * modes + s * KX + at, 8), 8), :] for s in range(slots)]
        place = iota((8, LANES), 1) // oc
        bit = 1
        while bit < slots:
            upper = (place // bit) % 2 == 1
            for s in range(slots):
                if not s & bit:
                    a, b = held[s], held[s | bit]
                    held[s] = jnp.where(upper, pltpu.roll(b, bit * oc, 1), a)
                    held[s | bit] = jnp.where(upper, b, pltpu.roll(a, LANES - bit * oc, 1))
            bit *= 2
        for s in range(slots):
            wt_ref[ri, s, pl.ds(pl.multiple_of(at, 8), 8), :] = held[s]
        return carry

    lax.fori_loop(0, 2 * (KX // 8), turn, 0)

    loaded("yh", "yl")
    pairs = 2 * rows
    a = xsend.shape[2] // 2
    total = pairs * a
    width = 2 * cells
    same = iota((pairs, a, width), 1) == (iota((pairs, a, width), 2) // (cells // a)) % a

    def expand(d, carry):
        for h, table in enumerate((yh_ref, yl_ref)):
            for l in range(kyl):
                full = jnp.where(same, table[d, l].astype(F32)[:, None, :], 0.0)
                yexp_ref[d, h, l * total:(l + 1) * total, :] = full.reshape(total, width).astype(BF16)
        return carry

    lax.fori_loop(0, cols, expand, 0)
    loaded("xf", "sel", "xb", "tz")
    for copy in y_copies:
        copy.wait_recv()

    deep = yrecv.shape[1] // a
    is_re = (iota((rows * a, LANES), 1) % rk) < rk // 2
    plain, cross = [], []
    for l in range(deep):
        u = yrecv[:, l * a:(l + 1) * a, :].reshape(rows * a, LANES)
        plain.append(u)
        cross.append(jnp.where(is_re, pltpu.roll(u, LANES - rk // 2, 1), -pltpu.roll(u, rk // 2, 1)))
    u = jnp.concatenate([jnp.concatenate(plain, 1), jnp.concatenate(cross, 1)], 0)
    high, low = split(u)
    both = dot(xf_ref[...], high)
    q = both[:KX] + both[KX:] + dot(xf_ref[0:KX, :], low)
    both = dot(stacked(q), sel_ref[...])
    amp_ref[...] = both[:KX] + both[KX:]
    origin = jnp.where((my_row == 0) & (my_col == 0), 1.0, 0.0)
    flag = jnp.where((iota((KX, LANES), 0) == 0) & (iota((KX, LANES), 1) < oc), origin, 0.0)

    x_copies = []
    for c in range(chunks):
        pr = wt_ref[0, c * group + width_in] * flag
        pi = wt_ref[1, c * group + width_in] * flag
        for j in range(width_in):
            wr, wi = wt_ref[0, c * group + j], wt_ref[1, c * group + j]
            ar = amp_ref[:, (2 * j) * LANES:(2 * j + 1) * LANES]
            ai = amp_ref[:, (2 * j + 1) * LANES:(2 * j + 2) * LANES]
            pr = pr + (wr * ar - wi * ai)
            pi = pi + (wr * ai + wi * ar)
        high, low = split(jnp.concatenate([pr, pi], 0))
        xsend[c] = dot(xb_ref[...], jnp.concatenate([high, low, high], 0)).reshape(xsend.shape[1:])
        x_copies.append([
            send(xsend.at[c, peer], xrecv.at[c, my_row], x_ss.at[c, i], x_rs.at[c, i], row=peer)
            for i, peer in enumerate(row_peers)
        ])
        xrecv[c, pl.ds(my_row, 1)] = xsend[c, pl.ds(my_row, 1)]

    tz = tz_ref[...]
    c_copies = []

    def landing(c):
        return dlast_ref if c == chunks - 1 else crecv.at[c]

    def inverse_y(c):
        for copy in x_copies[c]:
            copy.wait_recv()
        turned = jnp.transpose(xrecv[c].reshape(total, LANES))
        held = jnp.concatenate([turned[l * ko:(l + 1) * ko] for l in range(kyl)], 1)
        halves = stacked(held)
        at = pl.ds(pl.multiple_of(my_col * 2 * ko, 2 * ko), 2 * ko)
        started = []
        for i in list(range(1, cols)) + [0]:
            d = lax.rem(my_col + i, cols)
            both = dot(halves, yexp_ref[d, 0])
            acc = both[:ko] + both[ko:] + dot(halves[:ko], yexp_ref[d, 1])
            acc = jnp.concatenate([acc[:, v * cells:(v + 1) * cells] for v in range(2)], 0)
            if i == 0:
                landing(c)[at, :] = acc
            else:
                csend[c, i - 1] = acc
                started.append(
                    send(csend.at[c, i - 1], landing(c).at[at, :], c_ss.at[c, i - 1], c_rs.at[c, i - 1], col=d)
                )
        c_copies.append(started)

    def inverse_z(c):
        for copy in c_copies[c]:
            copy.wait_recv()
        for i in range(oc):
            o = c * oc + i
            row = lambda j: comb_ref[o:o + 1, j * LANES:(j + 1) * LANES]
            d = crecv[c, pl.ds(i, cols * 2 * kzl, stride=oc), :]
            feats_ref[o] = one_channel(d, row, adv_ref, tz)

    for c in range(chunks):
        inverse_y(c)
        if 0 <= c - lag < chunks - 1:
            inverse_z(c - lag)
    for c in range(max(chunks - lag, 0), chunks - 1):
        inverse_z(c)
    for copy in c_copies[chunks - 1]:
        copy.wait_recv()
    for copies in [z_copies, y_copies] + x_copies + c_copies:
        for copy in copies:
            copy.wait_send()


def finish_kernel(oc, depth, *refs):
    if len(refs) == 8:
        feats_ref, refs = refs[0], refs[1:]
        first = feats_ref.shape[0]
    else:
        feats_ref, first = None, 0
    d_ref, adv_ref, comb_ref, tz_ref, out_ref, last_ref, sems = refs
    copies = []
    if feats_ref is not None:
        copies.append(pltpu.make_async_copy(feats_ref, out_ref.at[pl.ds(0, first)], sems.at[oc]))
        copies[0].start()
    for i in range(oc):
        o = first + i
        row = lambda j: comb_ref[o:o + 1, j * LANES:(j + 1) * LANES]
        last_ref[i] = one_channel(d_ref[pl.ds(i, depth, stride=oc), :], row, adv_ref, tz_ref[...])
        copy = pltpu.make_async_copy(last_ref.at[pl.ds(i, 1)], out_ref.at[pl.ds(o, 1)], sems.at[i])
        copy.start()
        copies.append(copy)
    for copy in copies:
        copy.wait()


def per_device(
    velocity, tendency, step_size, lift_weight, lift_bias, spectral_weight, local_weight, local_bias
):
    samples, width_in, a, b, nz = velocity.shape
    channels = lift_weight.shape[0]
    rows, cols = lax.axis_size("row"), lax.axis_size("col")
    full_x, full_y = a * rows, b * cols
    kzl, kyl = KZ // cols, KY // rows
    slots = kyl * kzl
    modes = slots * KX
    cells = a * b
    group = width_in + 1
    oc = LANES // slots
    chunks = channels // oc
    ko = kzl * oc
    lag = 3
    vmem = pl.BlockSpec(memory_space=pltpu.VMEM)
    anywhere = pl.BlockSpec(memory_space=pl.ANY)
    stored = spectral_weight.reshape(2 * modes, channels * channels)

    zc, zs = trig(np.arange(KZ), nz)
    rk = 2 * max(kzl, 4)
    zf = np.zeros((cols, 2, rk // 2, nz), np.float32)
    zf[:, :, :kzl] = np.stack([zc, -zs], 0).reshape(2, cols, kzl, nz).transpose(1, 0, 2, 3)
    zf2 = np.concatenate(np_halves(zf.reshape(cols * rk, nz)), 0)
    yc, ys = trig(waves(KY), full_y)
    xc, xs = trig(waves(KX), full_x)
    scale = 1.0 / (full_x * full_y * nz)
    xf2 = np.concatenate(np_halves(np.concatenate([xc, xs], 1) * scale), 0)
    parts = 2
    deep = kyl // parts
    slot = LANES // parts
    yf = np.stack([yc, ys], 0).reshape(2, rows, deep, parts, 1, cols, 1, b)
    yf = yf * np.eye(a).reshape(1, 1, 1, 1, a, 1, a, 1)
    yf = yf.transpose(0, 3, 1, 2, 4, 5, 6, 7).reshape(2 * parts * rows * deep * a, cols * cells).T
    yfh, yfl = np_halves(yf)
    sel = np.zeros((deep, parts, slot, width_in, 2, kyl, kzl, oc), np.float32)
    for l in range(kyl):
        for j in range(width_in):
            for ri in range(2):
                for k in range(kzl):
                    sel[l // parts, l % parts, j * rk + ri * (rk // 2) + k, j, ri, l, k] = 1
    sel = sel.reshape(deep * LANES, width_in * 2 * LANES)
    xb = np.stack([np.stack([xc, -xs], 0), np.stack([xs, xc], 0)], 0)
    xb = xb.reshape(2, 2, KX, rows, a).transpose(3, 0, 4, 1, 2).reshape(rows * 2 * a, 2 * KX)
    xbh, xbl = np_halves(xb)
    xb3 = np.concatenate([xbh, xbh, xbl], 1)
    yb = np.stack([np.stack([yc, ys], 0), np.stack([-ys, yc], 0)], 0)
    yb = yb.reshape(2, 2, rows, kyl, cols, b).transpose(4, 3, 2, 0, 1, 5)
    yb = np.broadcast_to(yb[..., None, :], (cols, kyl, rows, 2, 2, a, b)).reshape(cols, kyl, rows * 2, 2 * cells)
    ybh, ybl = np_halves(yb)
    twice = np.where(np.arange(KZ) == 0, 1.0, 2.0)[:, None]
    zb = np.stack([twice * zc, -twice * zs], 0).reshape(2, cols, kzl, nz).transpose(1, 0, 2, 3).reshape(2 * KZ, nz)
    zbh, zbl = np_halves(zb)
    zb3 = np.concatenate([zbh, zbh, zbl], 0)
    tz = jnp.asarray(zb3)

    results = []
    for sample in range(samples):
        inputs = [
            velocity[sample].reshape(width_in, cells, nz), tendency[sample].reshape(width_in, cells, nz),
            step_size[sample].reshape(1, 1), lift_weight.T, lift_bias.reshape(1, channels), local_weight,
            local_bias.reshape(1, channels), jnp.asarray(zf2), jnp.asarray(yfh), jnp.asarray(yfl), jnp.asarray(xf2),
            jnp.asarray(sel, BF16), jnp.asarray(xb3), jnp.asarray(ybh), jnp.asarray(ybl), tz, stored,
        ]
        dma = lambda *shape: pltpu.SemaphoreType.DMA(shape)
        first = channels - oc
        outs = [
            jax.ShapeDtypeStruct((cols * 2 * ko, cells), F32),
            jax.ShapeDtypeStruct((width_in, cells, nz), F32),
            jax.ShapeDtypeStruct((channels, group * LANES), F32),
        ]
        if first:
            outs = [jax.ShapeDtypeStruct((first, cells, nz), BF16)] + outs
        held = pl.pallas_call(
            functools.partial(layer_kernel, kyl, kzl, oc, lag),
            out_shape=outs,
            in_specs=[anywhere] * len(inputs),
            out_specs=[vmem] * len(outs),
            scratch_shapes=[pltpu.VMEM(x.shape, x.dtype) for x in inputs] + [
                pltpu.VMEM((channels * channels, 2 * LANES), BF16),
                pltpu.VMEM((2 * modes, LANES), F32),
                pltpu.VMEM((2, slots, KX, LANES), F32),
                pltpu.VMEM((cols, 2, kyl * rows * 2 * a, 2 * cells), BF16),
                pltpu.VMEM((cols, width_in * rk, cells), F32),
                pltpu.VMEM((cols, width_in * rk, cells), F32),
                pltpu.VMEM((parts * slot, rows * deep * a), F32),
                pltpu.VMEM((rows, deep * a, LANES), F32),
                pltpu.VMEM((rows, deep * a, LANES), F32),
                pltpu.VMEM((KX, width_in * 2 * LANES), F32),
                pltpu.VMEM((chunks, rows, 2 * a, LANES), F32),
                pltpu.VMEM((chunks, rows, 2 * a, LANES), F32),
                pltpu.VMEM((chunks, cols - 1, 2 * ko, cells), F32),
                pltpu.VMEM((chunks, cols * 2 * ko, cells), F32),
                dma(len(inputs)),
                dma(cols - 1), dma(cols - 1), dma(rows - 1), dma(rows - 1),
                dma(chunks, rows - 1), dma(chunks, rows - 1), dma(chunks, cols - 1), dma(chunks, cols - 1),
            ],
            compiler_params=pltpu.CompilerParams(
                vmem_limit_bytes=40 * 1024 * 1024, collective_id=0, has_side_effects=True
            ),
        )(*[x if x.size == 1 else pltpu.with_memory_space_constraint(x, pltpu.HBM) for x in inputs])
        features = pl.pallas_call(
            functools.partial(finish_kernel, oc, cols * 2 * kzl),
            out_shape=jax.ShapeDtypeStruct((channels, cells, nz), BF16),
            in_specs=[vmem] * (len(held) + 1),
            out_specs=anywhere,
            scratch_shapes=[pltpu.VMEM((oc, cells, nz), BF16), dma(oc + 1)],
            compiler_params=pltpu.CompilerParams(vmem_limit_bytes=16 * 1024 * 1024),
        )(*held, tz)
        results.append(features.reshape(channels, a, b, nz))
    return jnp.stack(results, 0)


def solution(mesh):
    in_specs = (
        P(None, None, "row", "col", None),
        P(None, None, "row", "col", None),
        P(),
        P(),
        P(),
        P(None, "row", "col", None, None),
        P(),
        P(),
    )
    out_specs = P(None, None, "row", "col", None)
    return jax.shard_map(
        per_device, mesh=mesh, in_specs=in_specs, out_specs=out_specs, check_vma=False
    )
```

```python
import functools
import math

import jax
import jax.numpy as jnp
import numpy as np
from jax import lax
from jax.experimental import pallas as pl
from jax.experimental.pallas import tpu as pltpu
from jax.sharding import PartitionSpec as P

KX = 32
KY = 32
KZ = 32
LANES = 128
HIGHEST = lax.Precision.HIGHEST
F32 = jnp.float32
BF16 = jnp.bfloat16
MESH = pl.DeviceIdType.MESH


def waves(count):
    index = np.arange(count)
    return np.where(index < count // 2, index, index - count)


def trig(wave, length):
    angle = ((wave[:, None] * np.arange(length)[None, :]) % length) * (2.0 * math.pi / length)
    return np.cos(angle), np.sin(angle)


def np_halves(table):
    table = np.asarray(table, np.float32)
    high = table.astype(jnp.bfloat16)
    low = (table - high.astype(np.float32)).astype(jnp.bfloat16)
    return high, low


def split(x):
    high = x.astype(BF16)
    return high, (x - high.astype(F32)).astype(BF16)


def stacked(x):
    high = x.astype(BF16).astype(F32)
    return jnp.concatenate([high, x - high], 0).astype(BF16)


def dot(a, b):
    return jnp.dot(a, b, preferred_element_type=F32)


def dot_rows(a, b, precision=None):
    return lax.dot_general(a, b, (((0,), (0,)), ((), ())), precision=precision, preferred_element_type=F32)


def dot_lanes(a, b):
    return lax.dot_general(a, b, (((1,), (1,)), ((), ())), preferred_element_type=F32)


def iota(shape, axis):
    return lax.broadcasted_iota(jnp.int32, shape, axis)


def one_channel(d, row, adv_ref, tz):
    width_in = adv_ref.shape[0]
    d = d + jnp.where(iota(d.shape, 0) == 0, row(width_in), 0.0)
    high, low = split(d)
    x = dot_rows(jnp.concatenate([high, low, high], 0), tz)
    for j in range(width_in):
        weight = row(j)
        x = x + jnp.concatenate([weight] * (x.shape[1] // LANES), 1) * adv_ref[j]
    inner = x * (0.7978845608028654 + 0.035677408136300125 * (x * x))
    half = 0.5 * x
    return (half + half * jnp.tanh(inner)).astype(BF16)


def layer_kernel(
    kyl, kzl, oc, lag, ahead, at_xf, at_sel, at_xb, vel_any, tend_any, step_any, lw_any, lb_any, cw_any, cb_any, zf_any,
    yf_any, ye_any, tab_any, w_any, *rest,
):
    chunks = LANES // (oc * (lw_any.shape[0] + 1))
    if chunks > 1:
        feats_ref, rest = rest[0], rest[1:]
    else:
        feats_ref = None
    (
        dlast_ref, adv_ref, comb_ref, vel_ref, tend_ref, step_ref, lw_ref, lb_ref, cw_ref, cb_ref, zf_ref, yf_ref, ye_ref,
        tab_ref, w_ref, lift_ref, wl_ref, wt_ref, zsend, zrecv, ypad, ysend, yrecv, amp_ref, xsend, xrecv, csend, crecv,
        in_sems, send_sems, z_rs, y_rs, x_rs, c_rs,
    ) = rest
    rows, cols = lax.axis_size("row"), lax.axis_size("col")
    my_row, my_col = lax.axis_index("row"), lax.axis_index("col")
    width_in, cells, _ = vel_ref.shape
    channels = cw_ref.shape[0]
    group = width_in + 1
    freq = zf_ref.shape[0] // 2
    rk = freq // cols
    slots = kyl * kzl
    modes = slots * KX
    ko = kzl * oc
    early = 2

    loads = {}
    order = [
        ("vel", vel_any, vel_ref), ("tend", tend_any, tend_ref), ("step", step_any, step_ref), ("zf", zf_any, zf_ref),
        ("lw", lw_any, lw_ref), ("lb", lb_any, lb_ref), ("cw", cw_any, cw_ref), ("cb", cb_any, cb_ref),
        ("w", w_any, w_ref), ("yf", yf_any, yf_ref), ("tab", tab_any, tab_ref), ("ye", ye_any, ye_ref),
    ]
    for n, (name, source, target) in enumerate(order):
        loads[name] = pltpu.make_async_copy(source, target, in_sems.at[n])
        loads[name].start()

    def loaded(*names):
        for name in names:
            loads[name].wait()

    barrier = pltpu.get_barrier_semaphore()
    row_peers = [lax.rem(my_row + i, rows) for i in range(1, rows)]
    col_peers = [lax.rem(my_col + i, cols) for i in range(1, cols)]
    for peer in row_peers:
        pl.semaphore_signal(barrier, inc=1, device_id={"row": peer}, device_id_type=MESH)
    for peer in col_peers:
        pl.semaphore_signal(barrier, inc=1, device_id={"col": peer}, device_id_type=MESH)

    def send(source, target, sends, receives, **where):
        pltpu.make_async_remote_copy(source, target, sends, receives, device_id=where, device_id_type=MESH).start()

    def take(ref, semaphore):
        pltpu.make_async_copy(ref, ref, semaphore).wait()

    loaded("vel", "tend", "step", "zf")
    step = step_ref[0:1, 0:1]
    for j in range(width_in):
        adv = vel_ref[j] + step * tend_ref[j]
        adv_ref[j] = adv
        high, low = split(adv)
        both = dot_lanes(zf_ref[...], high)
        z = both[:freq] + both[freq:] + dot_lanes(zf_ref[0:freq, :], low)
        zsend[:, j * rk:(j + 1) * rk, :] = z.reshape(cols, rk, cells)
    pl.semaphore_wait(barrier, rows + cols - 2)
    for peer in col_peers:
        send(zsend.at[peer], zrecv.at[my_col], send_sems.at[0], z_rs, col=peer)
    zrecv[pl.ds(my_col, 1)] = zsend[pl.ds(my_col, 1)]

    loaded("lw", "lb", "cw", "cb")
    eight = iota((8, channels), 0)
    lift = jnp.where(eight == width_in, lb_ref[...], 0.0)
    for j in range(width_in):
        lift = jnp.where(eight == j, lw_ref[j:j + 1, :], lift)
    block = iota((8, LANES), 1) // oc
    pick = jnp.where(block % group == iota((8, LANES), 0), 1.0, 0.0)
    spread = dot_rows(lift, pick, HIGHEST)
    high = spread.astype(BF16).astype(F32)
    low = spread - high
    lane = iota((channels, LANES), 1)
    owner = (lane // (oc * group)) * oc + lane % oc
    for o in range(channels):
        at = slice(o * channels, (o + 1) * channels)
        lift_ref[at, :LANES] = jnp.where(owner == o, high, 0.0).astype(BF16)
        lift_ref[at, LANES:] = jnp.where(owner == o, low, 0.0).astype(BF16)
    wide = (8, group * LANES)
    spread = dot_rows(lift, jnp.where(iota(wide, 1) // LANES == iota(wide, 0), 1.0, 0.0), HIGHEST)
    comb = jnp.dot(cw_ref[...], spread, precision=HIGHEST, preferred_element_type=F32)
    bias = jnp.where(eight == 0, cb_ref[...], 0.0)
    bias = dot_rows(bias, jnp.where(iota((8, LANES), 0) == 0, 1.0, 0.0), HIGHEST)
    comb_ref[:, :width_in * LANES] = comb[:, :width_in * LANES]
    comb_ref[:, width_in * LANES:] = comb[:, width_in * LANES:] + bias

    loaded("w")
    step_rows = modes // 2

    def weigh(n):
        at = slice(n * step_rows, (n + 1) * step_rows)
        both = dot(w_ref[at, :], lift_ref[...])
        wl_ref[at, :] = both[:, :LANES] + both[:, LANES:]

    for n in range(4):
        weigh(n)

    def turn(n, carry):
        ri, at = n // (KX // 8), (n % (KX // 8)) * 8
        held = [wl_ref[pl.ds(pl.multiple_of(ri * modes + s * KX + at, 8), 8), :] for s in range(slots)]
        place = iota((8, LANES), 1) // oc
        bit = 1
        while bit < slots:
            upper = (place // bit) % 2 == 1
            for s in range(slots):
                if not s & bit:
                    a, b = held[s], held[s | bit]
                    held[s] = jnp.where(upper, pltpu.roll(b, bit * oc, 1), a)
                    held[s | bit] = jnp.where(upper, b, pltpu.roll(a, LANES - bit * oc, 1))
            bit *= 2
        for s in range(slots):
            wt_ref[ri, s, pl.ds(pl.multiple_of(at, 8), 8), :] = held[s]
        return carry

    lax.fori_loop(0, early, turn, 0)

    loaded("yf")
    take(zrecv.at[pl.ds(0, cols - 1)], z_rs)

    x = jnp.concatenate([zrecv[s] for s in range(cols)], 1)
    depth = width_in * rk
    halves = stacked(x)
    both = dot(halves, yf_ref[0])
    y = both[:depth] + both[depth:] + dot(x.astype(BF16), yf_ref[1])
    lanes = yf_ref.shape[2] // 2
    wide = ypad.shape[1]
    parts = lanes // wide
    slot = ypad.shape[0] // parts
    ypad[...] = jnp.zeros_like(ypad)
    low_rows = iota((rk, lanes), 0) < rk // 2
    for j in range(width_in):
        here = y[j * rk:(j + 1) * rk]
        turned = pltpu.roll(here[:, lanes:], rk // 2, 0)
        here = here[:, :lanes] + jnp.where(low_rows, turned, -turned)
        for p in range(parts):
            ypad[p * slot + j * rk:p * slot + (j + 1) * rk, :] = here[:, p * wide:(p + 1) * wide]
    ysend[...] = jnp.transpose(ypad[...]).reshape(ysend.shape)
    for peer in row_peers:
        send(ysend.at[peer], yrecv.at[my_row], send_sems.at[1], y_rs, row=peer)
    yrecv[pl.ds(my_row, 1)] = ysend[pl.ds(my_row, 1)]

    lax.fori_loop(early, 2 * (KX // 8), turn, 0)
    loaded("tab", "ye")
    take(yrecv.at[pl.ds(0, rows - 1)], y_rs)

    a = xsend.shape[3]
    deep = yrecv.shape[1] // a
    is_re = (iota((rows * a, LANES), 1) % rk) < rk // 2
    plain, cross = [], []
    for l in range(deep):
        u = yrecv[:, l * a:(l + 1) * a, :].reshape(rows * a, LANES)
        plain.append(u)
        cross.append(jnp.where(is_re, pltpu.roll(u, LANES - rk // 2, 1), -pltpu.roll(u, rk // 2, 1)))
    u = jnp.concatenate([jnp.concatenate(plain, 1), jnp.concatenate(cross, 1)], 0)
    high, low = split(u)
    xf = tab_ref[at_xf:at_xf + 2 * KX, :2 * rows * a]
    both = dot(xf, high)
    q = both[:KX] + both[KX:] + dot(xf[:KX], low)
    halves = stacked(q)
    for j in range(width_in):
        both = dot(halves, tab_ref[at_sel + j * deep * LANES:at_sel + (j + 1) * deep * LANES, :])
        amp_ref[:, 2 * j * LANES:(2 * j + 2) * LANES] = both[:KX] + both[KX:]
    origin = jnp.where((my_row == 0) & (my_col == 0), 1.0, 0.0)
    flag = jnp.where((iota((KX, LANES), 0) == 0) & (iota((KX, LANES), 1) < oc), origin, 0.0)

    xb = tab_ref[at_xb:at_xb + rows * 2 * a, :6 * KX]

    def mix(c):
        pr = wt_ref[0, c * group + width_in] * flag
        pi = wt_ref[1, c * group + width_in] * flag
        for j in range(width_in):
            wr, wi = wt_ref[0, c * group + j], wt_ref[1, c * group + j]
            ar = amp_ref[:, (2 * j) * LANES:(2 * j + 1) * LANES]
            ai = amp_ref[:, (2 * j + 1) * LANES:(2 * j + 2) * LANES]
            pr = pr + (wr * ar - wi * ai)
            pi = pi + (wr * ai + wi * ar)
        high, low = split(jnp.concatenate([pr, pi], 0))
        xsend[c] = dot(xb, jnp.concatenate([high, low, high], 0)).reshape(xsend.shape[1:])
        for peer in row_peers:
            send(xsend.at[c, peer], xrecv.at[c, my_row], send_sems.at[2], x_rs.at[c], row=peer)
        xrecv[c, pl.ds(my_row, 1)] = xsend[c, pl.ds(my_row, 1)]

    tz = tab_ref[0:6 * KZ, :]
    side = rows * a
    middle = cells // 2
    upper = iota((ko, LANES), 1) >= LANES // 2

    def swap(first, second):
        return (
            jnp.where(upper, pltpu.roll(second, LANES // 2, 1), first),
            jnp.where(upper, second, pltpu.roll(first, LANES // 2, 1)),
        )

    def landing(c):
        return dlast_ref if c == chunks - 1 else crecv.at[c]

    def inverse_y(c):
        take(xrecv.at[c, pl.ds(0, rows - 1)], x_rs.at[c])
        turned = jnp.concatenate([xrecv[c, :, h].reshape(side, LANES) for h in range(2)], 0)
        turned = jnp.transpose(turned)
        held = [turned[l * ko:(l + 1) * ko] for l in range(kyl)]
        if side == LANES:
            held = [jnp.concatenate([x[:, h * side:(h + 1) * side] for x in held], 1) for h in range(2)]
        else:
            tiles = [swap(held[l], held[l + 1]) for l in range(0, kyl, 2)]
            held = [jnp.concatenate([x[h] for x in tiles], 1) for h in range(2)]
        halves = stacked(jnp.concatenate(held, 0))
        at = pl.ds(pl.multiple_of(my_col * 2 * ko, 2 * ko), 2 * ko)
        for i in range(0, cols, 2):
            targets = [lax.rem(my_col + i + 1, cols), lax.rem(my_col + i + 2, cols)]
            both = dot(halves, jnp.concatenate([ye_ref[d, 0] for d in targets], 1))
            acc = both[:2 * ko] + both[2 * ko:]
            acc = acc + dot(halves[:2 * ko], jnp.concatenate([ye_ref[d, 1] for d in targets], 1))
            for n, d in enumerate(targets):
                here = acc[:, n * LANES:(n + 1) * LANES]
                here = jnp.concatenate(swap(here[:ko], here[ko:]), 0)
                if i + n == cols - 1:
                    landing(c)[at, :] = here
                else:
                    csend[c, i + n] = here
                    send(csend.at[c, i + n], landing(c).at[at, :], send_sems.at[3], c_rs.at[c], col=d)

    def arrive(c):
        take(landing(c).at[pl.ds(0, (cols - 1) * 2 * ko), :], c_rs.at[c])

    def inverse_z(c):
        arrive(c)
        for i in range(oc):
            o = c * oc + i
            row = lambda j: comb_ref[o:o + 1, j * LANES:(j + 1) * LANES]
            d = crecv[c, pl.ds(i, cols * 2 * kzl, stride=oc), :]
            feats_ref[o] = one_channel(d, row, adv_ref, tz)

    for c in range(min(ahead, chunks)):
        mix(c)
    for c in range(chunks):
        inverse_y(c)
        if c + ahead < chunks:
            mix(c + ahead)
        if 0 <= c - lag < chunks - 1:
            inverse_z(c - lag)
    for c in range(max(chunks - lag, 0), chunks - 1):
        inverse_z(c)
    arrive(chunks - 1)
    take(zsend.at[pl.ds(0, cols - 1)], send_sems.at[0])
    take(ysend.at[pl.ds(0, rows - 1)], send_sems.at[1])
    take(xsend.at[:, pl.ds(0, rows - 1)], send_sems.at[2])
    take(csend, send_sems.at[3])


def finish_kernel(oc, depth, *refs):
    if len(refs) == 8:
        feats_ref, refs = refs[0], refs[1:]
        first = feats_ref.shape[0]
    else:
        feats_ref, first = None, 0
    d_ref, adv_ref, comb_ref, tz_ref, out_ref, last_ref, sems = refs
    copies = []
    if feats_ref is not None:
        copies.append(pltpu.make_async_copy(feats_ref, out_ref.at[pl.ds(0, first)], sems.at[oc]))
        copies[0].start()
    for i in range(oc):
        o = first + i
        row = lambda j: comb_ref[o:o + 1, j * LANES:(j + 1) * LANES]
        last_ref[i] = one_channel(d_ref[pl.ds(i, depth, stride=oc), :], row, adv_ref, tz_ref[...])
        copy = pltpu.make_async_copy(last_ref.at[pl.ds(i, 1)], out_ref.at[pl.ds(o, 1)], sems.at[i])
        copy.start()
        copies.append(copy)
    for copy in copies:
        copy.wait()


def per_device(
    velocity, tendency, step_size, lift_weight, lift_bias, spectral_weight, local_weight, local_bias
):
    samples, width_in, a, b, nz = velocity.shape
    channels = lift_weight.shape[0]
    rows, cols = lax.axis_size("row"), lax.axis_size("col")
    full_x, full_y = a * rows, b * cols
    kzl, kyl = KZ // cols, KY // rows
    slots = kyl * kzl
    modes = slots * KX
    cells = a * b
    group = width_in + 1
    oc = LANES // slots
    chunks = channels // oc
    ko = kzl * oc
    lag, ahead = 3, 3
    vmem = pl.BlockSpec(memory_space=pltpu.VMEM)
    anywhere = pl.BlockSpec(memory_space=pl.ANY)
    stored = spectral_weight.reshape(2 * modes, channels * channels)

    zc, zs = trig(np.arange(KZ), nz)
    rk = 2 * max(kzl, 4)
    zf = np.zeros((cols, 2, rk // 2, nz), np.float32)
    zf[:, :, :kzl] = np.stack([zc, -zs], 0).reshape(2, cols, kzl, nz).transpose(1, 0, 2, 3)
    zf2 = np.concatenate(np_halves(zf.reshape(cols * rk, nz)), 0)
    yc, ys = trig(waves(KY), full_y)
    xc, xs = trig(waves(KX), full_x)
    scale = 1.0 / (full_x * full_y * nz)
    xf2 = np.concatenate(np_halves(np.concatenate([xc, xs], 1) * scale), 0)
    parts = 2
    deep = kyl // parts
    slot = LANES // parts
    yf = np.stack([yc, ys], 0).reshape(2, rows, deep, parts, 1, cols, 1, b)
    yf = yf * np.eye(a).reshape(1, 1, 1, 1, a, 1, a, 1)
    yf = yf.transpose(0, 3, 1, 2, 4, 5, 6, 7).reshape(2 * parts * rows * deep * a, cols * cells).T
    yf = np.stack(np_halves(yf), 0)
    sel = np.zeros((deep, parts, slot, width_in, 2, kyl, kzl, oc), np.float32)
    for l in range(kyl):
        for j in range(width_in):
            for ri in range(2):
                for k in range(kzl):
                    sel[l // parts, l % parts, j * rk + ri * (rk // 2) + k, j, ri, l, k] = 1
    sel = sel.reshape(deep * LANES, width_in * 2 * LANES)
    xb = np.stack([np.stack([xc, -xs], 0), np.stack([xs, xc], 0)], 0)
    xb = xb.reshape(2, 2, KX, rows, 2, a // 2).transpose(3, 4, 0, 5, 1, 2).reshape(rows * 2 * a, 2 * KX)
    xbh, xbl = np_halves(xb)
    xb3 = np.concatenate([xbh, xbh, xbl], 1)
    yb = np.stack([np.stack([yc, ys], 0), np.stack([-ys, yc], 0)], 0)
    yb = yb.reshape(2, 2, rows, kyl, cols, b).transpose(4, 3, 2, 0, 1, 5)
    yb = yb.reshape(cols, kyl, rows, 2, 1, 2, 1, b) * np.eye(a // 2).reshape(a // 2, 1, a // 2, 1)
    ye = np.stack(np_halves(yb.reshape(cols, kyl * rows * a, cells)), 1)
    twice = np.where(np.arange(KZ) == 0, 1.0, 2.0)[:, None]
    zb = np.stack([twice * zc, -twice * zs], 0).reshape(2, cols, kzl, nz).transpose(1, 0, 2, 3).reshape(2 * KZ, nz)
    zbh, zbl = np_halves(zb)
    zb3 = np.concatenate([zbh, zbh, zbl], 0)
    tz = jnp.asarray(zb3)
    sel = sel.reshape(deep * LANES, width_in, 2 * LANES).transpose(1, 0, 2).reshape(-1, 2 * LANES)
    pieces = [zb3, xf2, sel, xb3]
    table = np.concatenate([np.pad(np.asarray(x, jnp.bfloat16), ((0, 0), (0, nz - x.shape[1]))) for x in pieces], 0)
    starts = [zb3.shape[0], zb3.shape[0] + xf2.shape[0], zb3.shape[0] + xf2.shape[0] + sel.shape[0]]

    results = []
    for sample in range(samples):
        inputs = [
            velocity[sample].reshape(width_in, cells, nz), tendency[sample].reshape(width_in, cells, nz),
            step_size[sample].reshape(1, 1), lift_weight.T, lift_bias.reshape(1, channels), local_weight,
            local_bias.reshape(1, channels), jnp.asarray(zf2), jnp.asarray(yf), jnp.asarray(ye), jnp.asarray(table), stored,
        ]
        dma = lambda *shape: pltpu.SemaphoreType.DMA(shape)
        first = channels - oc
        outs = [
            jax.ShapeDtypeStruct((cols * 2 * ko, cells), F32),
            jax.ShapeDtypeStruct((width_in, cells, nz), F32),
            jax.ShapeDtypeStruct((channels, group * LANES), F32),
        ]
        if first:
            outs = [jax.ShapeDtypeStruct((first, cells, nz), BF16)] + outs
        held = pl.pallas_call(
            functools.partial(layer_kernel, kyl, kzl, oc, lag, ahead, *starts),
            out_shape=outs,
            in_specs=[anywhere] * len(inputs),
            out_specs=[vmem] * len(outs),
            scratch_shapes=[pltpu.VMEM(x.shape, x.dtype) for x in inputs] + [
                pltpu.VMEM((channels * channels, 2 * LANES), BF16),
                pltpu.VMEM((2 * modes, LANES), F32),
                pltpu.VMEM((2, slots, KX, LANES), F32),
                pltpu.VMEM((cols, width_in * rk, cells), F32),
                pltpu.VMEM((cols, width_in * rk, cells), F32),
                pltpu.VMEM((parts * slot, rows * deep * a), F32),
                pltpu.VMEM((rows, deep * a, LANES), F32),
                pltpu.VMEM((rows, deep * a, LANES), F32),
                pltpu.VMEM((KX, width_in * 2 * LANES), F32),
                pltpu.VMEM((chunks, rows, 2, a, LANES), F32),
                pltpu.VMEM((chunks, rows, 2, a, LANES), F32),
                pltpu.VMEM((chunks, cols - 1, 2 * ko, cells), F32),
                pltpu.VMEM((chunks, cols * 2 * ko, cells), F32),
                dma(len(inputs)), dma(4), pltpu.SemaphoreType.DMA, pltpu.SemaphoreType.DMA, dma(chunks), dma(chunks),
            ],
            compiler_params=pltpu.CompilerParams(
                vmem_limit_bytes=40 * 1024 * 1024, collective_id=0, has_side_effects=True
            ),
        )(*[x if x.size == 1 else pltpu.with_memory_space_constraint(x, pltpu.HBM) for x in inputs])
        features = pl.pallas_call(
            functools.partial(finish_kernel, oc, cols * 2 * kzl),
            out_shape=jax.ShapeDtypeStruct((channels, cells, nz), BF16),
            in_specs=[vmem] * (len(held) + 1),
            out_specs=anywhere,
            scratch_shapes=[pltpu.VMEM((oc, cells, nz), BF16), dma(oc + 1)],
            compiler_params=pltpu.CompilerParams(vmem_limit_bytes=16 * 1024 * 1024),
        )(*held, tz)
        results.append(features.reshape(channels, a, b, nz))
    return jnp.stack(results, 0)


def solution(mesh):
    in_specs = (
        P(None, None, "row", "col", None),
        P(None, None, "row", "col", None),
        P(),
        P(),
        P(),
        P(None, "row", "col", None, None),
        P(),
        P(),
    )
    out_specs = P(None, None, "row", "col", None)
    return jax.shard_map(
        per_device, mesh=mesh, in_specs=in_specs, out_specs=out_specs, check_vma=False
    )
```

```python
import functools
import math

import jax
import jax.numpy as jnp
import numpy as np
from jax import lax
from jax.experimental import pallas as pl
from jax.experimental.pallas import tpu as pltpu
from jax.sharding import PartitionSpec as P

KX = 32
KY = 32
KZ = 32
LANES = 128
HIGHEST = lax.Precision.HIGHEST
F32 = jnp.float32
BF16 = jnp.bfloat16
MESH = pl.DeviceIdType.MESH


def waves(count):
    index = np.arange(count)
    return np.where(index < count // 2, index, index - count)


def trig(wave, length):
    angle = ((wave[:, None] * np.arange(length)[None, :]) % length) * (2.0 * math.pi / length)
    return np.cos(angle), np.sin(angle)


def np_halves(table):
    table = np.asarray(table, np.float32)
    high = table.astype(jnp.bfloat16)
    low = (table - high.astype(np.float32)).astype(jnp.bfloat16)
    return high, low


def split(x):
    high = x.astype(BF16)
    return high, (x - high.astype(F32)).astype(BF16)


def stacked(x):
    high = x.astype(BF16).astype(F32)
    return jnp.concatenate([high, x - high], 0).astype(BF16)


def dot(a, b):
    return jnp.dot(a, b, preferred_element_type=F32)


def dot_rows(a, b, precision=None):
    return lax.dot_general(a, b, (((0,), (0,)), ((), ())), precision=precision, preferred_element_type=F32)


def dot_lanes(a, b):
    return lax.dot_general(a, b, (((1,), (1,)), ((), ())), preferred_element_type=F32)


def iota(shape, axis):
    return lax.broadcasted_iota(jnp.int32, shape, axis)


def one_channel(d, row, adv_ref, tz):
    width_in = adv_ref.shape[0]
    d = d + jnp.where(iota(d.shape, 0) == 0, row(width_in), 0.0)
    high, low = split(d)
    x = dot_rows(jnp.concatenate([high, low, high], 0), tz)
    for j in range(width_in):
        weight = row(j)
        x = x + jnp.concatenate([weight] * (x.shape[1] // LANES), 1) * adv_ref[j]
    inner = x * (0.7978845608028654 + 0.035677408136300125 * (x * x))
    half = 0.5 * x
    return (half + half * jnp.tanh(inner)).astype(BF16)


def layer_kernel(
    kyl, kzl, oc, lag, ahead, at_xf, at_sel, at_xb, vel_any, tend_any, step_any, lw_any, lb_any, cw_any, cb_any, zf_any,
    yf_any, ye_any, tab_any, w_any, *rest,
):
    chunks = LANES // (oc * (lw_any.shape[0] + 1))
    if chunks > 1:
        feats_ref, rest = rest[0], rest[1:]
    else:
        feats_ref = None
    (
        dlast_ref, adv_ref, comb_ref, vel_ref, tend_ref, step_ref, lw_ref, lb_ref, cw_ref, cb_ref, zf_ref, yf_ref, ye_ref,
        tab_ref, w_ref, lift_ref, wl_ref, wt_ref, zsend, zrecv, ypad, ysend, yrecv, amp_ref, xsend, xrecv, csend, crecv,
        in_sems, send_sems, z_rs, y_rs, x_rs, c_rs,
    ) = rest
    rows, cols = lax.axis_size("row"), lax.axis_size("col")
    my_row, my_col = lax.axis_index("row"), lax.axis_index("col")
    width_in, cells, _ = vel_ref.shape
    channels = cw_ref.shape[0]
    group = width_in + 1
    freq = zf_ref.shape[0] // 2
    rk = freq // cols
    slots = kyl * kzl
    modes = slots * KX
    ko = kzl * oc
    early = 2

    loads = {}
    order = [
        ("vel", vel_any, vel_ref), ("tend", tend_any, tend_ref), ("step", step_any, step_ref), ("zf", zf_any, zf_ref),
        ("lw", lw_any, lw_ref), ("lb", lb_any, lb_ref), ("cw", cw_any, cw_ref), ("cb", cb_any, cb_ref),
        ("w", w_any, w_ref), ("yf", yf_any, yf_ref), ("tab", tab_any, tab_ref), ("ye", ye_any, ye_ref),
    ]
    for n, (name, source, target) in enumerate(order):
        loads[name] = pltpu.make_async_copy(source, target, in_sems.at[n])
        loads[name].start()

    def loaded(*names):
        for name in names:
            loads[name].wait()

    barrier = pltpu.get_barrier_semaphore()
    row_peers = [lax.rem(my_row + i, rows) for i in range(1, rows)]
    col_peers = [lax.rem(my_col + i, cols) for i in range(1, cols)]
    for peer in row_peers:
        pl.semaphore_signal(barrier, inc=1, device_id={"row": peer}, device_id_type=MESH)
    for peer in col_peers:
        pl.semaphore_signal(barrier, inc=1, device_id={"col": peer}, device_id_type=MESH)

    def send(source, target, sends, receives, **where):
        pltpu.make_async_remote_copy(source, target, sends, receives, device_id=where, device_id_type=MESH).start()

    def take(ref, semaphore):
        pltpu.make_async_copy(ref, ref, semaphore).wait()

    loaded("vel", "tend", "step", "zf")
    step = step_ref[0:1, 0:1]
    for j in range(width_in):
        adv = vel_ref[j] + step * tend_ref[j]
        adv_ref[j] = adv
        high, low = split(adv)
        both = dot_lanes(zf_ref[...], high)
        z = both[:freq] + both[freq:] + dot_lanes(zf_ref[0:freq, :], low)
        zsend[:, j * rk:(j + 1) * rk, :] = z.reshape(cols, rk, cells)
    pl.semaphore_wait(barrier, rows + cols - 2)
    for peer in col_peers:
        send(zsend.at[peer], zrecv.at[my_col], send_sems.at[0], z_rs, col=peer)
    zrecv[pl.ds(my_col, 1)] = zsend[pl.ds(my_col, 1)]

    loaded("lw", "lb", "cw", "cb")
    eight = iota((8, channels), 0)
    lift = jnp.where(eight == width_in, lb_ref[...], 0.0)
    for j in range(width_in):
        lift = jnp.where(eight == j, lw_ref[j:j + 1, :], lift)
    block = iota((8, LANES), 1) // oc
    pick = jnp.where(block % group == iota((8, LANES), 0), 1.0, 0.0)
    spread = dot_rows(lift, pick, HIGHEST)
    high = spread.astype(BF16).astype(F32)
    low = spread - high
    lane = iota((channels, LANES), 1)
    owner = (lane // (oc * group)) * oc + lane % oc
    for o in range(channels):
        at = slice(o * channels, (o + 1) * channels)
        lift_ref[at, :LANES] = jnp.where(owner == o, high, 0.0).astype(BF16)
        lift_ref[at, LANES:] = jnp.where(owner == o, low, 0.0).astype(BF16)
    wide = (8, group * LANES)
    spread = dot_rows(lift, jnp.where(iota(wide, 1) // LANES == iota(wide, 0), 1.0, 0.0), HIGHEST)
    comb = jnp.dot(cw_ref[...], spread, precision=HIGHEST, preferred_element_type=F32)
    bias = jnp.where(eight == 0, cb_ref[...], 0.0)
    bias = dot_rows(bias, jnp.where(iota((8, LANES), 0) == 0, 1.0, 0.0), HIGHEST)
    comb_ref[:, :width_in * LANES] = comb[:, :width_in * LANES]
    comb_ref[:, width_in * LANES:] = comb[:, width_in * LANES:] + bias

    loaded("w")
    step_rows = modes // 2

    def weigh(n):
        at = slice(n * step_rows, (n + 1) * step_rows)
        both = dot(w_ref[at, :], lift_ref[...])
        wl_ref[at, :] = both[:, :LANES] + both[:, LANES:]

    for n in range(4):
        weigh(n)

    def turn(n, carry):
        ri, at = n // (KX // 8), (n % (KX // 8)) * 8
        held = [wl_ref[pl.ds(pl.multiple_of(ri * modes + s * KX + at, 8), 8), :] for s in range(slots)]
        place = iota((8, LANES), 1) // oc
        bit = 1
        while bit < slots:
            upper = (place // bit) % 2 == 1
            for s in range(slots):
                if not s & bit:
                    a, b = held[s], held[s | bit]
                    held[s] = jnp.where(upper, pltpu.roll(b, bit * oc, 1), a)
                    held[s | bit] = jnp.where(upper, b, pltpu.roll(a, LANES - bit * oc, 1))
            bit *= 2
        for s in range(slots):
            wt_ref[ri, s, pl.ds(pl.multiple_of(at, 8), 8), :] = held[s]
        return carry

    lax.fori_loop(0, early, turn, 0)

    loaded("yf")
    take(zrecv.at[pl.ds(0, cols - 1)], z_rs)

    x = jnp.concatenate([zrecv[s] for s in range(cols)], 1)
    depth = width_in * rk
    halves = stacked(x)
    both = dot(halves, yf_ref[0])
    y = both[:depth] + both[depth:] + dot(x.astype(BF16), yf_ref[1])
    lanes = yf_ref.shape[2] // 2
    wide = ypad.shape[1]
    parts = lanes // wide
    slot = ypad.shape[0] // parts
    ypad[...] = jnp.zeros_like(ypad)
    low_rows = iota((rk, lanes), 0) < rk // 2
    for j in range(width_in):
        here = y[j * rk:(j + 1) * rk]
        turned = pltpu.roll(here[:, lanes:], rk // 2, 0)
        here = here[:, :lanes] + jnp.where(low_rows, turned, -turned)
        for p in range(parts):
            ypad[p * slot + j * rk:p * slot + (j + 1) * rk, :] = here[:, p * wide:(p + 1) * wide]
    ysend[...] = jnp.transpose(ypad[...]).reshape(ysend.shape)
    for peer in row_peers:
        send(ysend.at[peer], yrecv.at[my_row], send_sems.at[1], y_rs, row=peer)
    yrecv[pl.ds(my_row, 1)] = ysend[pl.ds(my_row, 1)]

    lax.fori_loop(early, 2 * (KX // 8), turn, 0)
    loaded("tab", "ye")
    take(yrecv.at[pl.ds(0, rows - 1)], y_rs)

    a = xsend.shape[3]
    deep = yrecv.shape[1] // a
    is_re = (iota((rows * a, LANES), 1) % rk) < rk // 2
    plain, cross = [], []
    for l in range(deep):
        u = yrecv[:, l * a:(l + 1) * a, :].reshape(rows * a, LANES)
        plain.append(u)
        cross.append(jnp.where(is_re, pltpu.roll(u, LANES - rk // 2, 1), -pltpu.roll(u, rk // 2, 1)))
    u = jnp.concatenate([jnp.concatenate(plain, 1), jnp.concatenate(cross, 1)], 0)
    high, low = split(u)
    xf = tab_ref[at_xf:at_xf + 2 * KX, :2 * rows * a]
    both = dot(xf, high)
    q = both[:KX] + both[KX:] + dot(xf[:KX], low)
    halves = stacked(q)
    for j in range(width_in):
        both = dot(halves, tab_ref[at_sel + j * deep * LANES:at_sel + (j + 1) * deep * LANES, :])
        amp_ref[:, 2 * j * LANES:(2 * j + 2) * LANES] = both[:KX] + both[KX:]
    origin = jnp.where((my_row == 0) & (my_col == 0), 1.0, 0.0)
    flag = jnp.where((iota((KX, LANES), 0) == 0) & (iota((KX, LANES), 1) < oc), origin, 0.0)

    xb = tab_ref[at_xb:at_xb + rows * 2 * a, :6 * KX]

    def mix(c):
        pr = wt_ref[0, c * group + width_in] * flag
        pi = wt_ref[1, c * group + width_in] * flag
        for j in range(width_in):
            wr, wi = wt_ref[0, c * group + j], wt_ref[1, c * group + j]
            ar = amp_ref[:, (2 * j) * LANES:(2 * j + 1) * LANES]
            ai = amp_ref[:, (2 * j + 1) * LANES:(2 * j + 2) * LANES]
            pr = pr + (wr * ar - wi * ai)
            pi = pi + (wr * ai + wi * ar)
        high, low = split(jnp.concatenate([pr, pi], 0))
        xsend[c] = dot(xb, jnp.concatenate([high, low, high], 0)).reshape(xsend.shape[1:])
        for peer in row_peers:
            send(xsend.at[c, peer], xrecv.at[c, my_row], send_sems.at[2], x_rs.at[c], row=peer)
        xrecv[c, pl.ds(my_row, 1)] = xsend[c, pl.ds(my_row, 1)]

    tz = tab_ref[0:6 * KZ, :]
    side = rows * a
    middle = cells // 2
    upper = iota((ko, LANES), 1) >= LANES // 2

    def swap(first, second):
        return (
            jnp.where(upper, pltpu.roll(second, LANES // 2, 1), first),
            jnp.where(upper, second, pltpu.roll(first, LANES // 2, 1)),
        )

    def landing(c):
        return dlast_ref if c == chunks - 1 else crecv.at[c]

    def inverse_y(c):
        take(xrecv.at[c, pl.ds(0, rows - 1)], x_rs.at[c])
        turned = jnp.concatenate([xrecv[c, :, h].reshape(side, LANES) for h in range(2)], 0)
        turned = jnp.transpose(turned)
        held = [turned[l * ko:(l + 1) * ko] for l in range(kyl)]
        if side == LANES:
            held = [jnp.concatenate([x[:, h * side:(h + 1) * side] for x in held], 1) for h in range(2)]
        else:
            tiles = [swap(held[l], held[l + 1]) for l in range(0, kyl, 2)]
            held = [jnp.concatenate([x[h] for x in tiles], 1) for h in range(2)]
        halves = stacked(jnp.concatenate(held, 0))
        at = pl.ds(pl.multiple_of(my_col * 2 * ko, 2 * ko), 2 * ko)
        for i in range(0, cols, 2):
            targets = [lax.rem(my_col + i + 1, cols), lax.rem(my_col + i + 2, cols)]
            both = dot(halves, jnp.concatenate([ye_ref[d, 0] for d in targets], 1))
            acc = both[:2 * ko] + both[2 * ko:]
            acc = acc + dot(halves[:2 * ko], jnp.concatenate([ye_ref[d, 1] for d in targets], 1))
            for n, d in enumerate(targets):
                here = acc[:, n * LANES:(n + 1) * LANES]
                here = jnp.concatenate(swap(here[:ko], here[ko:]), 0)
                if i + n == cols - 1:
                    landing(c)[at, :] = here
                else:
                    csend[c, i + n] = here
                    send(csend.at[c, i + n], landing(c).at[at, :], send_sems.at[3], c_rs.at[c], col=d)

    def arrive(c):
        take(landing(c).at[pl.ds(0, (cols - 1) * 2 * ko), :], c_rs.at[c])

    def inverse_z(c):
        arrive(c)
        for i in range(oc):
            o = c * oc + i
            row = lambda j: comb_ref[o:o + 1, j * LANES:(j + 1) * LANES]
            d = crecv[c, pl.ds(i, cols * 2 * kzl, stride=oc), :]
            feats_ref[o] = one_channel(d, row, adv_ref, tz)

    for c in range(min(ahead, chunks)):
        mix(c)
    for c in range(chunks):
        inverse_y(c)
        if c + ahead < chunks:
            mix(c + ahead)
        if 0 <= c - lag < chunks - 1:
            inverse_z(c - lag)
    for c in range(max(chunks - lag, 0), chunks - 1):
        inverse_z(c)
    arrive(chunks - 1)
    take(zsend.at[pl.ds(0, cols - 1)], send_sems.at[0])
    take(ysend.at[pl.ds(0, rows - 1)], send_sems.at[1])
    take(xsend.at[:, pl.ds(0, rows - 1)], send_sems.at[2])
    take(csend, send_sems.at[3])


def finish_kernel(oc, depth, *refs):
    if len(refs) == 8:
        feats_ref, refs = refs[0], refs[1:]
        first = feats_ref.shape[0]
    else:
        feats_ref, first = None, 0
    d_ref, adv_ref, comb_ref, tz_ref, out_ref, last_ref, sems = refs
    copies = []
    if feats_ref is not None:
        copies.append(pltpu.make_async_copy(feats_ref, out_ref.at[pl.ds(0, first)], sems.at[oc]))
        copies[0].start()
    for i in range(oc):
        o = first + i
        row = lambda j: comb_ref[o:o + 1, j * LANES:(j + 1) * LANES]
        last_ref[i] = one_channel(d_ref[pl.ds(i, depth, stride=oc), :], row, adv_ref, tz_ref[...])
        copy = pltpu.make_async_copy(last_ref.at[pl.ds(i, 1)], out_ref.at[pl.ds(o, 1)], sems.at[i])
        copy.start()
        copies.append(copy)
    for copy in copies:
        copy.wait()


def per_device(
    velocity, tendency, step_size, lift_weight, lift_bias, spectral_weight, local_weight, local_bias
):
    samples, width_in, a, b, nz = velocity.shape
    channels = lift_weight.shape[0]
    rows, cols = lax.axis_size("row"), lax.axis_size("col")
    full_x, full_y = a * rows, b * cols
    kzl, kyl = KZ // cols, KY // rows
    slots = kyl * kzl
    modes = slots * KX
    cells = a * b
    group = width_in + 1
    oc = LANES // slots
    chunks = channels // oc
    ko = kzl * oc
    lag, ahead = 3, 4
    vmem = pl.BlockSpec(memory_space=pltpu.VMEM)
    anywhere = pl.BlockSpec(memory_space=pl.ANY)
    stored = spectral_weight.reshape(2 * modes, channels * channels)

    zc, zs = trig(np.arange(KZ), nz)
    rk = 2 * max(kzl, 4)
    zf = np.zeros((cols, 2, rk // 2, nz), np.float32)
    zf[:, :, :kzl] = np.stack([zc, -zs], 0).reshape(2, cols, kzl, nz).transpose(1, 0, 2, 3)
    zf2 = np.concatenate(np_halves(zf.reshape(cols * rk, nz)), 0)
    yc, ys = trig(waves(KY), full_y)
    xc, xs = trig(waves(KX), full_x)
    scale = 1.0 / (full_x * full_y * nz)
    xf2 = np.concatenate(np_halves(np.concatenate([xc, xs], 1) * scale), 0)
    parts = 2
    deep = kyl // parts
    slot = LANES // parts
    yf = np.stack([yc, ys], 0).reshape(2, rows, deep, parts, 1, cols, 1, b)
    yf = yf * np.eye(a).reshape(1, 1, 1, 1, a, 1, a, 1)
    yf = yf.transpose(0, 3, 1, 2, 4, 5, 6, 7).reshape(2 * parts * rows * deep * a, cols * cells).T
    yf = np.stack(np_halves(yf), 0)
    sel = np.zeros((deep, parts, slot, width_in, 2, kyl, kzl, oc), np.float32)
    for l in range(kyl):
        for j in range(width_in):
            for ri in range(2):
                for k in range(kzl):
                    sel[l // parts, l % parts, j * rk + ri * (rk // 2) + k, j, ri, l, k] = 1
    sel = sel.reshape(deep * LANES, width_in * 2 * LANES)
    xb = np.stack([np.stack([xc, -xs], 0), np.stack([xs, xc], 0)], 0)
    xb = xb.reshape(2, 2, KX, rows, 2, a // 2).transpose(3, 4, 0, 5, 1, 2).reshape(rows * 2 * a, 2 * KX)
    xbh, xbl = np_halves(xb)
    xb3 = np.concatenate([xbh, xbh, xbl], 1)
    yb = np.stack([np.stack([yc, ys], 0), np.stack([-ys, yc], 0)], 0)
    yb = yb.reshape(2, 2, rows, kyl, cols, b).transpose(4, 3, 2, 0, 1, 5)
    yb = yb.reshape(cols, kyl, rows, 2, 1, 2, 1, b) * np.eye(a // 2).reshape(a // 2, 1, a // 2, 1)
    ye = np.stack(np_halves(yb.reshape(cols, kyl * rows * a, cells)), 1)
    twice = np.where(np.arange(KZ) == 0, 1.0, 2.0)[:, None]
    zb = np.stack([twice * zc, -twice * zs], 0).reshape(2, cols, kzl, nz).transpose(1, 0, 2, 3).reshape(2 * KZ, nz)
    zbh, zbl = np_halves(zb)
    zb3 = np.concatenate([zbh, zbh, zbl], 0)
    tz = jnp.asarray(zb3)
    sel = sel.reshape(deep * LANES, width_in, 2 * LANES).transpose(1, 0, 2).reshape(-1, 2 * LANES)
    pieces = [zb3, xf2, sel, xb3]
    table = np.concatenate([np.pad(np.asarray(x, jnp.bfloat16), ((0, 0), (0, nz - x.shape[1]))) for x in pieces], 0)
    starts = [zb3.shape[0], zb3.shape[0] + xf2.shape[0], zb3.shape[0] + xf2.shape[0] + sel.shape[0]]

    results = []
    for sample in range(samples):
        inputs = [
            velocity[sample].reshape(width_in, cells, nz), tendency[sample].reshape(width_in, cells, nz),
            step_size[sample].reshape(1, 1), lift_weight.T, lift_bias.reshape(1, channels), local_weight,
            local_bias.reshape(1, channels), jnp.asarray(zf2), jnp.asarray(yf), jnp.asarray(ye), jnp.asarray(table), stored,
        ]
        dma = lambda *shape: pltpu.SemaphoreType.DMA(shape)
        first = channels - oc
        outs = [
            jax.ShapeDtypeStruct((cols * 2 * ko, cells), F32),
            jax.ShapeDtypeStruct((width_in, cells, nz), F32),
            jax.ShapeDtypeStruct((channels, group * LANES), F32),
        ]
        if first:
            outs = [jax.ShapeDtypeStruct((first, cells, nz), BF16)] + outs
        held = pl.pallas_call(
            functools.partial(layer_kernel, kyl, kzl, oc, lag, ahead, *starts),
            out_shape=outs,
            in_specs=[anywhere] * len(inputs),
            out_specs=[vmem] * len(outs),
            scratch_shapes=[pltpu.VMEM(x.shape, x.dtype) for x in inputs] + [
                pltpu.VMEM((channels * channels, 2 * LANES), BF16),
                pltpu.VMEM((2 * modes, LANES), F32),
                pltpu.VMEM((2, slots, KX, LANES), F32),
                pltpu.VMEM((cols, width_in * rk, cells), F32),
                pltpu.VMEM((cols, width_in * rk, cells), F32),
                pltpu.VMEM((parts * slot, rows * deep * a), F32),
                pltpu.VMEM((rows, deep * a, LANES), F32),
                pltpu.VMEM((rows, deep * a, LANES), F32),
                pltpu.VMEM((KX, width_in * 2 * LANES), F32),
                pltpu.VMEM((chunks, rows, 2, a, LANES), F32),
                pltpu.VMEM((chunks, rows, 2, a, LANES), F32),
                pltpu.VMEM((chunks, cols - 1, 2 * ko, cells), F32),
                pltpu.VMEM((chunks, cols * 2 * ko, cells), F32),
                dma(len(inputs)), dma(4), pltpu.SemaphoreType.DMA, pltpu.SemaphoreType.DMA, dma(chunks), dma(chunks),
            ],
            compiler_params=pltpu.CompilerParams(
                vmem_limit_bytes=40 * 1024 * 1024, collective_id=0, has_side_effects=True
            ),
        )(*[x if x.size == 1 else pltpu.with_memory_space_constraint(x, pltpu.HBM) for x in inputs])
        features = pl.pallas_call(
            functools.partial(finish_kernel, oc, cols * 2 * kzl),
            out_shape=jax.ShapeDtypeStruct((channels, cells, nz), BF16),
            in_specs=[vmem] * (len(held) + 1),
            out_specs=anywhere,
            scratch_shapes=[pltpu.VMEM((oc, cells, nz), BF16), dma(oc + 1)],
            compiler_params=pltpu.CompilerParams(vmem_limit_bytes=16 * 1024 * 1024),
        )(*held, tz)
        results.append(features.reshape(channels, a, b, nz))
    return jnp.stack(results, 0)


def solution(mesh):
    in_specs = (
        P(None, None, "row", "col", None),
        P(None, None, "row", "col", None),
        P(),
        P(),
        P(),
        P(None, "row", "col", None, None),
        P(),
        P(),
    )
    out_specs = P(None, None, "row", "col", None)
    return jax.shard_map(
        per_device, mesh=mesh, in_specs=in_specs, out_specs=out_specs, check_vma=False
    )
```

```python
import functools
import math

import jax
import jax.numpy as jnp
import numpy as np
from jax import lax
from jax.experimental import pallas as pl
from jax.experimental.pallas import tpu as pltpu
from jax.sharding import PartitionSpec as P

KX = 32
KY = 32
KZ = 32
LANES = 128
HIGHEST = lax.Precision.HIGHEST
F32 = jnp.float32
BF16 = jnp.bfloat16
MESH = pl.DeviceIdType.MESH


def waves(count):
    index = np.arange(count)
    return np.where(index < count // 2, index, index - count)


def trig(wave, length):
    angle = ((wave[:, None] * np.arange(length)[None, :]) % length) * (2.0 * math.pi / length)
    return np.cos(angle), np.sin(angle)


def np_halves(table):
    table = np.asarray(table, np.float32)
    high = table.astype(jnp.bfloat16)
    low = (table - high.astype(np.float32)).astype(jnp.bfloat16)
    return high, low


def split(x):
    high = x.astype(BF16)
    return high, (x - high.astype(F32)).astype(BF16)


def stacked(x):
    high = x.astype(BF16).astype(F32)
    return jnp.concatenate([high, x - high], 0).astype(BF16)


def dot(a, b):
    return jnp.dot(a, b, preferred_element_type=F32)


def dot_rows(a, b, precision=None):
    return lax.dot_general(a, b, (((0,), (0,)), ((), ())), precision=precision, preferred_element_type=F32)


def dot_lanes(a, b):
    return lax.dot_general(a, b, (((1,), (1,)), ((), ())), preferred_element_type=F32)


def iota(shape, axis):
    return lax.broadcasted_iota(jnp.int32, shape, axis)


def one_channel(d, row, adv_ref, tz):
    width_in = adv_ref.shape[0]
    d = d + jnp.where(iota(d.shape, 0) == 0, row(width_in), 0.0)
    high, low = split(d)
    x = dot_rows(jnp.concatenate([high, low, high], 0), tz)
    for j in range(width_in):
        weight = row(j)
        x = x + jnp.concatenate([weight] * (x.shape[1] // LANES), 1) * adv_ref[j]
    inner = x * (0.7978845608028654 + 0.035677408136300125 * (x * x))
    half = 0.5 * x
    return (half + half * jnp.tanh(inner)).astype(BF16)


def layer_kernel(
    kyl, kzl, oc, lag, ahead, at_xf, at_sel, at_xb, vel_any, tend_any, step_any, lw_any, lb_any, cw_any, cb_any, zf_any,
    yf_any, ye_any, tab_any, w_any, *rest,
):
    chunks = LANES // (oc * (lw_any.shape[0] + 1))
    if chunks > 1:
        feats_ref, rest = rest[0], rest[1:]
    else:
        feats_ref = None
    (
        dlast_ref, adv_ref, comb_ref, vel_ref, tend_ref, step_ref, lw_ref, lb_ref, cw_ref, cb_ref, zf_ref, yf_ref, ye_ref,
        tab_ref, w_ref, lift_ref, wl_ref, wt_ref, zsend, zrecv, ypad, ysend, yrecv, amp_ref, xsend, xrecv, csend, crecv,
        in_sems, send_sems, z_rs, y_rs, x_rs, c_rs,
    ) = rest
    rows, cols = lax.axis_size("row"), lax.axis_size("col")
    my_row, my_col = lax.axis_index("row"), lax.axis_index("col")
    width_in, cells, _ = vel_ref.shape
    channels = cw_ref.shape[0]
    group = width_in + 1
    freq = zf_ref.shape[0] // 2
    rk = freq // cols
    slots = kyl * kzl
    modes = slots * KX
    ko = kzl * oc
    early = 4

    loads = {}
    order = [
        ("vel", vel_any, vel_ref), ("tend", tend_any, tend_ref), ("step", step_any, step_ref), ("zf", zf_any, zf_ref),
        ("lw", lw_any, lw_ref), ("lb", lb_any, lb_ref), ("cw", cw_any, cw_ref), ("cb", cb_any, cb_ref),
        ("w", w_any, w_ref), ("yf", yf_any, yf_ref), ("tab", tab_any, tab_ref), ("ye", ye_any, ye_ref),
    ]
    for n, (name, source, target) in enumerate(order):
        loads[name] = pltpu.make_async_copy(source, target, in_sems.at[n])
        loads[name].start()

    def loaded(*names):
        for name in names:
            loads[name].wait()

    barrier = pltpu.get_barrier_semaphore()
    row_peers = [lax.rem(my_row + i, rows) for i in range(1, rows)]
    col_peers = [lax.rem(my_col + i, cols) for i in range(1, cols)]
    for peer in row_peers:
        pl.semaphore_signal(barrier, inc=1, device_id={"row": peer}, device_id_type=MESH)
    for peer in col_peers:
        pl.semaphore_signal(barrier, inc=1, device_id={"col": peer}, device_id_type=MESH)

    def send(source, target, sends, receives, **where):
        pltpu.make_async_remote_copy(source, target, sends, receives, device_id=where, device_id_type=MESH).start()

    def take(ref, semaphore):
        pltpu.make_async_copy(ref, ref, semaphore).wait()

    def send_z(j):
        at = pl.ds(j * rk, rk)
        for peer in col_peers:
            send(zsend.at[peer, at], zrecv.at[my_col, at], send_sems.at[0], z_rs, col=peer)

    loaded("vel", "tend", "step", "zf")
    step = step_ref[0:1, 0:1]
    for j in range(width_in):
        adv = vel_ref[j] + step * tend_ref[j]
        adv_ref[j] = adv
        high, low = split(adv)
        both = dot_lanes(zf_ref[...], high)
        z = both[:freq] + both[freq:] + dot_lanes(zf_ref[0:freq, :], low)
        zsend[:, j * rk:(j + 1) * rk, :] = z.reshape(cols, rk, cells)
        if j == 0:
            pl.semaphore_wait(barrier, rows + cols - 2)
        send_z(j)
    zrecv[pl.ds(my_col, 1)] = zsend[pl.ds(my_col, 1)]

    loaded("lw", "lb", "cw", "cb")
    eight = iota((8, channels), 0)
    lift = jnp.where(eight == width_in, lb_ref[...], 0.0)
    for j in range(width_in):
        lift = jnp.where(eight == j, lw_ref[j:j + 1, :], lift)
    block = iota((8, LANES), 1) // oc
    pick = jnp.where(block % group == iota((8, LANES), 0), 1.0, 0.0)
    spread = dot_rows(lift, pick, HIGHEST)
    high = spread.astype(BF16).astype(F32)
    low = spread - high
    lane = iota((channels, LANES), 1)
    owner = (lane // (oc * group)) * oc + lane % oc
    for o in range(channels):
        at = slice(o * channels, (o + 1) * channels)
        lift_ref[at, :LANES] = jnp.where(owner == o, high, 0.0).astype(BF16)
        lift_ref[at, LANES:] = jnp.where(owner == o, low, 0.0).astype(BF16)
    wide = (8, group * LANES)
    spread = dot_rows(lift, jnp.where(iota(wide, 1) // LANES == iota(wide, 0), 1.0, 0.0), HIGHEST)
    comb = jnp.dot(cw_ref[...], spread, precision=HIGHEST, preferred_element_type=F32)
    bias = jnp.where(eight == 0, cb_ref[...], 0.0)
    bias = dot_rows(bias, jnp.where(iota((8, LANES), 0) == 0, 1.0, 0.0), HIGHEST)
    comb_ref[:, :width_in * LANES] = comb[:, :width_in * LANES]
    comb_ref[:, width_in * LANES:] = comb[:, width_in * LANES:] + bias

    loaded("w")
    step_rows = modes // 2

    def weigh(n):
        at = slice(n * step_rows, (n + 1) * step_rows)
        both = dot(w_ref[at, :], lift_ref[...])
        wl_ref[at, :] = both[:, :LANES] + both[:, LANES:]

    for n in range(4):
        weigh(n)

    def turn(n, carry):
        ri, at = n // (KX // 8), (n % (KX // 8)) * 8
        held = [wl_ref[pl.ds(pl.multiple_of(ri * modes + s * KX + at, 8), 8), :] for s in range(slots)]
        held = [pltpu.roll(x, s * oc, 1) if s else x for s, x in enumerate(held)]
        held = [held[-s % slots] for s in range(slots)]
        place = iota((8, LANES), 1) // oc
        bit = 1
        while bit < slots:
            upper = (place // bit) % 2 == 1
            held = [jnp.where(upper, held[(s - bit) % slots], held[s]) for s in range(slots)]
            bit *= 2
        held = [pltpu.roll(x, LANES - s * oc, 1) if s else x for s, x in enumerate(held)]
        for s in range(slots):
            wt_ref[ri, s, pl.ds(pl.multiple_of(at, 8), 8), :] = held[s]
        return carry

    lax.fori_loop(0, early, turn, 0)

    loaded("yf")
    take(zrecv.at[pl.ds(0, cols - 1)], z_rs)

    x = jnp.concatenate([zrecv[s] for s in range(cols)], 1)
    depth = width_in * rk
    halves = stacked(x)
    both = dot(halves, yf_ref[0])
    y = both[:depth] + both[depth:] + dot(x.astype(BF16), yf_ref[1])
    lanes = yf_ref.shape[2] // 2
    wide = ypad.shape[1]
    parts = lanes // wide
    slot = ypad.shape[0] // parts
    ypad[...] = jnp.zeros_like(ypad)
    low_rows = iota((rk, lanes), 0) < rk // 2
    for j in range(width_in):
        here = y[j * rk:(j + 1) * rk]
        turned = pltpu.roll(here[:, lanes:], rk // 2, 0)
        here = here[:, :lanes] + jnp.where(low_rows, turned, -turned)
        for p in range(parts):
            ypad[p * slot + j * rk:p * slot + (j + 1) * rk, :] = here[:, p * wide:(p + 1) * wide]
    ysend[...] = jnp.transpose(ypad[...]).reshape(ysend.shape)
    for peer in row_peers:
        send(ysend.at[peer], yrecv.at[my_row], send_sems.at[1], y_rs, row=peer)
    yrecv[pl.ds(my_row, 1)] = ysend[pl.ds(my_row, 1)]

    lax.fori_loop(early, 2 * (KX // 8), turn, 0)
    loaded("tab", "ye")
    take(yrecv.at[pl.ds(0, rows - 1)], y_rs)

    a = xsend.shape[3]
    deep = yrecv.shape[1] // a
    is_re = (iota((rows * a, LANES), 1) % rk) < rk // 2
    plain, cross = [], []
    for l in range(deep):
        u = yrecv[:, l * a:(l + 1) * a, :].reshape(rows * a, LANES)
        plain.append(u)
        cross.append(jnp.where(is_re, pltpu.roll(u, LANES - rk // 2, 1), -pltpu.roll(u, rk // 2, 1)))
    u = jnp.concatenate([jnp.concatenate(plain, 1), jnp.concatenate(cross, 1)], 0)
    high, low = split(u)
    xf = tab_ref[at_xf:at_xf + 2 * KX, :2 * rows * a]
    both = dot(xf, high)
    q = both[:KX] + both[KX:] + dot(xf[:KX], low)
    halves = stacked(q)
    for j in range(width_in):
        both = dot(halves, tab_ref[at_sel + j * deep * LANES:at_sel + (j + 1) * deep * LANES, :])
        amp_ref[:, 2 * j * LANES:(2 * j + 2) * LANES] = both[:KX] + both[KX:]
    origin = jnp.where((my_row == 0) & (my_col == 0), 1.0, 0.0)
    flag = jnp.where((iota((KX, LANES), 0) == 0) & (iota((KX, LANES), 1) < oc), origin, 0.0)

    xb = tab_ref[at_xb:at_xb + rows * 2 * a, :6 * KX]

    def mix(c):
        pr = wt_ref[0, c * group + width_in] * flag
        pi = wt_ref[1, c * group + width_in] * flag
        for j in range(width_in):
            wr, wi = wt_ref[0, c * group + j], wt_ref[1, c * group + j]
            ar = amp_ref[:, (2 * j) * LANES:(2 * j + 1) * LANES]
            ai = amp_ref[:, (2 * j + 1) * LANES:(2 * j + 2) * LANES]
            pr = pr + (wr * ar - wi * ai)
            pi = pi + (wr * ai + wi * ar)
        high, low = split(jnp.concatenate([pr, pi], 0))
        xsend[c] = dot(xb, jnp.concatenate([high, low, high], 0)).reshape(xsend.shape[1:])
        for peer in row_peers:
            send(xsend.at[c, peer], xrecv.at[c, my_row], send_sems.at[2], x_rs.at[c], row=peer)
        xrecv[c, pl.ds(my_row, 1)] = xsend[c, pl.ds(my_row, 1)]

    tz = tab_ref[0:6 * KZ, :]
    side = rows * a
    middle = cells // 2
    upper = iota((ko, LANES), 1) >= LANES // 2

    def swap(first, second):
        return (
            jnp.where(upper, pltpu.roll(second, LANES // 2, 1), first),
            jnp.where(upper, second, pltpu.roll(first, LANES // 2, 1)),
        )

    def landing(c):
        return dlast_ref if c == chunks - 1 else crecv.at[c]

    def inverse_y(c):
        take(xrecv.at[c, pl.ds(0, rows - 1)], x_rs.at[c])
        turned = jnp.concatenate([xrecv[c, :, h].reshape(side, LANES) for h in range(2)], 0)
        turned = jnp.transpose(turned)
        held = [turned[l * ko:(l + 1) * ko] for l in range(kyl)]
        if side == LANES:
            held = [jnp.concatenate([x[:, h * side:(h + 1) * side] for x in held], 1) for h in range(2)]
        else:
            tiles = [swap(held[l], held[l + 1]) for l in range(0, kyl, 2)]
            held = [jnp.concatenate([x[h] for x in tiles], 1) for h in range(2)]
        halves = stacked(jnp.concatenate(held, 0))
        at = pl.ds(pl.multiple_of(my_col * 2 * ko, 2 * ko), 2 * ko)
        for i in range(0, cols, 2):
            targets = [lax.rem(my_col + i + 1, cols), lax.rem(my_col + i + 2, cols)]
            both = dot(halves, jnp.concatenate([ye_ref[d, 0] for d in targets], 1))
            acc = both[:2 * ko] + both[2 * ko:]
            acc = acc + dot(halves[:2 * ko], jnp.concatenate([ye_ref[d, 1] for d in targets], 1))
            for n, d in enumerate(targets):
                here = acc[:, n * LANES:(n + 1) * LANES]
                here = jnp.concatenate(swap(here[:ko], here[ko:]), 0)
                if i + n == cols - 1:
                    landing(c)[at, :] = here
                else:
                    csend[c, i + n] = here
                    send(csend.at[c, i + n], landing(c).at[at, :], send_sems.at[3], c_rs.at[c], col=d)

    def arrive(c):
        take(landing(c).at[pl.ds(0, (cols - 1) * 2 * ko), :], c_rs.at[c])

    def inverse_z(c):
        arrive(c)
        for i in range(oc):
            o = c * oc + i
            row = lambda j: comb_ref[o:o + 1, j * LANES:(j + 1) * LANES]
            d = crecv[c, pl.ds(i, cols * 2 * kzl, stride=oc), :]
            feats_ref[o] = one_channel(d, row, adv_ref, tz)

    for c in range(min(ahead, chunks)):
        mix(c)
    for c in range(chunks):
        inverse_y(c)
        if c + ahead < chunks:
            mix(c + ahead)
        if 0 <= c - lag < chunks - 1:
            inverse_z(c - lag)
    for c in range(max(chunks - lag, 0), chunks - 1):
        inverse_z(c)
    arrive(chunks - 1)
    take(zsend.at[pl.ds(0, cols - 1)], send_sems.at[0])
    take(ysend.at[pl.ds(0, rows - 1)], send_sems.at[1])
    take(xsend.at[:, pl.ds(0, rows - 1)], send_sems.at[2])
    take(csend, send_sems.at[3])


def finish_kernel(oc, depth, *refs):
    if len(refs) == 8:
        feats_ref, refs = refs[0], refs[1:]
        first = feats_ref.shape[0]
    else:
        feats_ref, first = None, 0
    d_ref, adv_ref, comb_ref, tz_ref, out_ref, last_ref, sems = refs
    copies = []
    if feats_ref is not None:
        copies.append(pltpu.make_async_copy(feats_ref, out_ref.at[pl.ds(0, first)], sems.at[oc]))
        copies[0].start()
    for i in range(oc):
        o = first + i
        row = lambda j: comb_ref[o:o + 1, j * LANES:(j + 1) * LANES]
        last_ref[i] = one_channel(d_ref[pl.ds(i, depth, stride=oc), :], row, adv_ref, tz_ref[...])
        copy = pltpu.make_async_copy(last_ref.at[pl.ds(i, 1)], out_ref.at[pl.ds(o, 1)], sems.at[i])
        copy.start()
        copies.append(copy)
    for copy in copies:
        copy.wait()


def per_device(
    velocity, tendency, step_size, lift_weight, lift_bias, spectral_weight, local_weight, local_bias
):
    samples, width_in, a, b, nz = velocity.shape
    channels = lift_weight.shape[0]
    rows, cols = lax.axis_size("row"), lax.axis_size("col")
    full_x, full_y = a * rows, b * cols
    kzl, kyl = KZ // cols, KY // rows
    slots = kyl * kzl
    modes = slots * KX
    cells = a * b
    group = width_in + 1
    oc = LANES // slots
    chunks = channels // oc
    ko = kzl * oc
    lag, ahead = 3, 4
    vmem = pl.BlockSpec(memory_space=pltpu.VMEM)
    anywhere = pl.BlockSpec(memory_space=pl.ANY)
    stored = spectral_weight.reshape(2 * modes, channels * channels)

    zc, zs = trig(np.arange(KZ), nz)
    rk = 2 * max(kzl, 4)
    zf = np.zeros((cols, 2, rk // 2, nz), np.float32)
    zf[:, :, :kzl] = np.stack([zc, -zs], 0).reshape(2, cols, kzl, nz).transpose(1, 0, 2, 3)
    zf2 = np.concatenate(np_halves(zf.reshape(cols * rk, nz)), 0)
    yc, ys = trig(waves(KY), full_y)
    xc, xs = trig(waves(KX), full_x)
    scale = 1.0 / (full_x * full_y * nz)
    xf2 = np.concatenate(np_halves(np.concatenate([xc, xs], 1) * scale), 0)
    parts = 2
    deep = kyl // parts
    slot = LANES // parts
    yf = np.stack([yc, ys], 0).reshape(2, rows, deep, parts, 1, cols, 1, b)
    yf = yf * np.eye(a).reshape(1, 1, 1, 1, a, 1, a, 1)
    yf = yf.transpose(0, 3, 1, 2, 4, 5, 6, 7).reshape(2 * parts * rows * deep * a, cols * cells).T
    yf = np.stack(np_halves(yf), 0)
    sel = np.zeros((deep, parts, slot, width_in, 2, kyl, kzl, oc), np.float32)
    for l in range(kyl):
        for j in range(width_in):
            for ri in range(2):
                for k in range(kzl):
                    sel[l // parts, l % parts, j * rk + ri * (rk // 2) + k, j, ri, l, k] = 1
    sel = sel.reshape(deep * LANES, width_in * 2 * LANES)
    xb = np.stack([np.stack([xc, -xs], 0), np.stack([xs, xc], 0)], 0)
    xb = xb.reshape(2, 2, KX, rows, 2, a // 2).transpose(3, 4, 0, 5, 1, 2).reshape(rows * 2 * a, 2 * KX)
    xbh, xbl = np_halves(xb)
    xb3 = np.concatenate([xbh, xbh, xbl], 1)
    yb = np.stack([np.stack([yc, ys], 0), np.stack([-ys, yc], 0)], 0)
    yb = yb.reshape(2, 2, rows, kyl, cols, b).transpose(4, 3, 2, 0, 1, 5)
    yb = yb.reshape(cols, kyl, rows, 2, 1, 2, 1, b) * np.eye(a // 2).reshape(a // 2, 1, a // 2, 1)
    ye = np.stack(np_halves(yb.reshape(cols, kyl * rows * a, cells)), 1)
    twice = np.where(np.arange(KZ) == 0, 1.0, 2.0)[:, None]
    zb = np.stack([twice * zc, -twice * zs], 0).reshape(2, cols, kzl, nz).transpose(1, 0, 2, 3).reshape(2 * KZ, nz)
    zbh, zbl = np_halves(zb)
    zb3 = np.concatenate([zbh, zbh, zbl], 0)
    tz = jnp.asarray(zb3)
    sel = sel.reshape(deep * LANES, width_in, 2 * LANES).transpose(1, 0, 2).reshape(-1, 2 * LANES)
    pieces = [zb3, xf2, sel, xb3]
    table = np.concatenate([np.pad(np.asarray(x, jnp.bfloat16), ((0, 0), (0, nz - x.shape[1]))) for x in pieces], 0)
    starts = [zb3.shape[0], zb3.shape[0] + xf2.shape[0], zb3.shape[0] + xf2.shape[0] + sel.shape[0]]

    results = []
    for sample in range(samples):
        inputs = [
            velocity[sample].reshape(width_in, cells, nz), tendency[sample].reshape(width_in, cells, nz),
            step_size[sample].reshape(1, 1), lift_weight.T, lift_bias.reshape(1, channels), local_weight,
            local_bias.reshape(1, channels), jnp.asarray(zf2), jnp.asarray(yf), jnp.asarray(ye), jnp.asarray(table), stored,
        ]
        dma = lambda *shape: pltpu.SemaphoreType.DMA(shape)
        first = channels - oc
        outs = [
            jax.ShapeDtypeStruct((cols * 2 * ko, cells), F32),
            jax.ShapeDtypeStruct((width_in, cells, nz), F32),
            jax.ShapeDtypeStruct((channels, group * LANES), F32),
        ]
        if first:
            outs = [jax.ShapeDtypeStruct((first, cells, nz), BF16)] + outs
        held = pl.pallas_call(
            functools.partial(layer_kernel, kyl, kzl, oc, lag, ahead, *starts),
            out_shape=outs,
            in_specs=[anywhere] * len(inputs),
            out_specs=[vmem] * len(outs),
            scratch_shapes=[pltpu.VMEM(x.shape, x.dtype) for x in inputs] + [
                pltpu.VMEM((channels * channels, 2 * LANES), BF16),
                pltpu.VMEM((2 * modes, LANES), F32),
                pltpu.VMEM((2, slots, KX, LANES), F32),
                pltpu.VMEM((cols, width_in * rk, cells), F32),
                pltpu.VMEM((cols, width_in * rk, cells), F32),
                pltpu.VMEM((parts * slot, rows * deep * a), F32),
                pltpu.VMEM((rows, deep * a, LANES), F32),
                pltpu.VMEM((rows, deep * a, LANES), F32),
                pltpu.VMEM((KX, width_in * 2 * LANES), F32),
                pltpu.VMEM((chunks, rows, 2, a, LANES), F32),
                pltpu.VMEM((chunks, rows, 2, a, LANES), F32),
                pltpu.VMEM((chunks, cols - 1, 2 * ko, cells), F32),
                pltpu.VMEM((chunks, cols * 2 * ko, cells), F32),
                dma(len(inputs)), dma(4), pltpu.SemaphoreType.DMA, pltpu.SemaphoreType.DMA, dma(chunks), dma(chunks),
            ],
            compiler_params=pltpu.CompilerParams(
                vmem_limit_bytes=40 * 1024 * 1024, collective_id=0, has_side_effects=True
            ),
        )(*[x if x.size == 1 else pltpu.with_memory_space_constraint(x, pltpu.HBM) for x in inputs])
        features = pl.pallas_call(
            functools.partial(finish_kernel, oc, cols * 2 * kzl),
            out_shape=jax.ShapeDtypeStruct((channels, cells, nz), BF16),
            in_specs=[vmem] * (len(held) + 1),
            out_specs=anywhere,
            scratch_shapes=[pltpu.VMEM((oc, cells, nz), BF16), dma(oc + 1)],
            compiler_params=pltpu.CompilerParams(vmem_limit_bytes=16 * 1024 * 1024),
        )(*held, tz)
        results.append(features.reshape(channels, a, b, nz))
    return jnp.stack(results, 0)


def solution(mesh):
    in_specs = (
        P(None, None, "row", "col", None),
        P(None, None, "row", "col", None),
        P(),
        P(),
        P(),
        P(None, "row", "col", None, None),
        P(),
        P(),
    )
    out_specs = P(None, None, "row", "col", None)
    return jax.shard_map(
        per_device, mesh=mesh, in_specs=in_specs, out_specs=out_specs, check_vma=False
    )
```

```python
import functools
import math

import jax
import jax.numpy as jnp
import numpy as np
from jax import lax
from jax.experimental import pallas as pl
from jax.experimental.pallas import tpu as pltpu
from jax.sharding import PartitionSpec as P

KX = 32
KY = 32
KZ = 32
LANES = 128
HIGHEST = lax.Precision.HIGHEST
F32 = jnp.float32
BF16 = jnp.bfloat16
MESH = pl.DeviceIdType.MESH


def waves(count):
    index = np.arange(count)
    return np.where(index < count // 2, index, index - count)


def trig(wave, length):
    angle = ((wave[:, None] * np.arange(length)[None, :]) % length) * (2.0 * math.pi / length)
    return np.cos(angle), np.sin(angle)


def np_halves(table):
    table = np.asarray(table, np.float32)
    high = table.astype(jnp.bfloat16)
    low = (table - high.astype(np.float32)).astype(jnp.bfloat16)
    return high, low


def split(x):
    high = x.astype(BF16)
    return high, (x - high.astype(F32)).astype(BF16)


def stacked(x):
    high = x.astype(BF16).astype(F32)
    return jnp.concatenate([high, x - high], 0).astype(BF16)


def dot(a, b):
    return jnp.dot(a, b, preferred_element_type=F32)


def dot_rows(a, b, precision=None):
    return lax.dot_general(a, b, (((0,), (0,)), ((), ())), precision=precision, preferred_element_type=F32)


def dot_lanes(a, b):
    return lax.dot_general(a, b, (((1,), (1,)), ((), ())), preferred_element_type=F32)


def iota(shape, axis):
    return lax.broadcasted_iota(jnp.int32, shape, axis)


def one_channel(d, row, adv_ref, tz):
    width_in = adv_ref.shape[0]
    d = d + jnp.where(iota(d.shape, 0) == 0, row(width_in), 0.0)
    high, low = split(d)
    x = dot_rows(jnp.concatenate([high, low, high], 0), tz)
    for j in range(width_in):
        weight = row(j)
        x = x + jnp.concatenate([weight] * (x.shape[1] // LANES), 1) * adv_ref[j]
    inner = x * (0.7978845608028654 + 0.035677408136300125 * (x * x))
    half = 0.5 * x
    return (half + half * jnp.tanh(inner)).astype(BF16)


def layer_kernel(
    kyl, kzl, oc, lag, ahead, at_xf, at_sel, at_xb, vel_any, tend_any, step_any, lw_any, lb_any, cw_any, cb_any, zf_any,
    yf_any, ye_any, tab_any, w_any, *rest,
):
    chunks = LANES // (oc * (lw_any.shape[0] + 1))
    if chunks > 1:
        feats_ref, rest = rest[0], rest[1:]
    else:
        feats_ref = None
    (
        dlast_ref, adv_ref, comb_ref, vel_ref, tend_ref, step_ref, lw_ref, lb_ref, cw_ref, cb_ref, zf_ref, yf_ref, ye_ref,
        tab_ref, w_ref, lift_ref, wl_ref, wt_ref, zsend, zrecv, ypad, ysend, yrecv, amp_ref, xsend, xrecv, csend, crecv,
        in_sems, send_sems, z_rs, y_rs, x_rs, c_rs,
    ) = rest
    rows, cols = lax.axis_size("row"), lax.axis_size("col")
    my_row, my_col = lax.axis_index("row"), lax.axis_index("col")
    width_in, cells, _ = vel_ref.shape
    channels = cw_ref.shape[0]
    group = width_in + 1
    freq = zf_ref.shape[0] // 2
    rk = freq // cols
    slots = kyl * kzl
    modes = slots * KX
    ko = kzl * oc
    early = 4

    loads = {}
    order = [
        ("vel", vel_any, vel_ref), ("tend", tend_any, tend_ref), ("step", step_any, step_ref), ("zf", zf_any, zf_ref),
        ("lw", lw_any, lw_ref), ("lb", lb_any, lb_ref), ("cw", cw_any, cw_ref), ("cb", cb_any, cb_ref),
        ("w", w_any, w_ref), ("yf", yf_any, yf_ref), ("tab", tab_any, tab_ref), ("ye", ye_any, ye_ref),
    ]
    for n, (name, source, target) in enumerate(order):
        loads[name] = pltpu.make_async_copy(source, target, in_sems.at[n])
        loads[name].start()

    def loaded(*names):
        for name in names:
            loads[name].wait()

    barrier = pltpu.get_barrier_semaphore()
    row_peers = [lax.rem(my_row + i, rows) for i in range(1, rows)]
    col_peers = [lax.rem(my_col + i, cols) for i in range(1, cols)]
    for peer in row_peers:
        pl.semaphore_signal(barrier, inc=1, device_id={"row": peer}, device_id_type=MESH)
    for peer in col_peers:
        pl.semaphore_signal(barrier, inc=1, device_id={"col": peer}, device_id_type=MESH)

    def send(source, target, sends, receives, **where):
        pltpu.make_async_remote_copy(source, target, sends, receives, device_id=where, device_id_type=MESH).start()

    def take(ref, semaphore):
        pltpu.make_async_copy(ref, ref, semaphore).wait()

    def send_z(j):
        at = pl.ds(j * rk, rk)
        for peer in col_peers:
            send(zsend.at[peer, at], zrecv.at[my_col, at], send_sems.at[0], z_rs, col=peer)

    loaded("vel", "tend", "step", "zf")
    step = step_ref[0:1, 0:1]
    for j in range(width_in):
        adv = vel_ref[j] + step * tend_ref[j]
        adv_ref[j] = adv
        high, low = split(adv)
        both = dot_lanes(zf_ref[...], high)
        z = both[:freq] + both[freq:] + dot_lanes(zf_ref[0:freq, :], low)
        zsend[:, j * rk:(j + 1) * rk, :] = z.reshape(cols, rk, cells)
        if j == 0:
            pl.semaphore_wait(barrier, rows + cols - 2)
        send_z(j)
    zrecv[pl.ds(my_col, 1)] = zsend[pl.ds(my_col, 1)]

    loaded("lw", "lb", "cw", "cb")
    eight = iota((8, channels), 0)
    lift = jnp.where(eight == width_in, lb_ref[...], 0.0)
    for j in range(width_in):
        lift = jnp.where(eight == j, lw_ref[j:j + 1, :], lift)
    block = iota((8, LANES), 1) // oc
    pick = jnp.where(block % group == iota((8, LANES), 0), 1.0, 0.0)
    spread = dot_rows(lift, pick, HIGHEST)
    high = spread.astype(BF16).astype(F32)
    low = spread - high
    lane = iota((channels, LANES), 1)
    owner = (lane // (oc * group)) * oc + lane % oc
    for o in range(channels):
        at = slice(o * channels, (o + 1) * channels)
        lift_ref[at, :LANES] = jnp.where(owner == o, high, 0.0).astype(BF16)
        lift_ref[at, LANES:] = jnp.where(owner == o, low, 0.0).astype(BF16)
    wide = (8, group * LANES)
    spread = dot_rows(lift, jnp.where(iota(wide, 1) // LANES == iota(wide, 0), 1.0, 0.0), HIGHEST)
    comb = jnp.dot(cw_ref[...], spread, precision=HIGHEST, preferred_element_type=F32)
    bias = jnp.where(eight == 0, cb_ref[...], 0.0)
    bias = dot_rows(bias, jnp.where(iota((8, LANES), 0) == 0, 1.0, 0.0), HIGHEST)
    comb_ref[:, :width_in * LANES] = comb[:, :width_in * LANES]
    comb_ref[:, width_in * LANES:] = comb[:, width_in * LANES:] + bias

    loaded("w")
    step_rows = modes // 2

    def weigh(n):
        at = slice(n * step_rows, (n + 1) * step_rows)
        both = dot(w_ref[at, :], lift_ref[...])
        wl_ref[at, :] = both[:, :LANES] + both[:, LANES:]

    for n in range(4):
        weigh(n)

    def turn(n, carry):
        ri, at = n // (KX // 8), (n % (KX // 8)) * 8
        held = [wl_ref[pl.ds(pl.multiple_of(ri * modes + s * KX + at, 8), 8), :] for s in range(slots)]
        held = [pltpu.roll(x, s * oc, 1) if s else x for s, x in enumerate(held)]
        held = [held[-s % slots] for s in range(slots)]
        place = iota((8, LANES), 1) // oc
        bit = 1
        while bit < slots:
            upper = (place // bit) % 2 == 1
            held = [jnp.where(upper, held[(s - bit) % slots], held[s]) for s in range(slots)]
            bit *= 2
        held = [pltpu.roll(x, LANES - s * oc, 1) if s else x for s, x in enumerate(held)]
        for s in range(slots):
            wt_ref[ri, s, pl.ds(pl.multiple_of(at, 8), 8), :] = held[s]
        return carry

    lax.fori_loop(0, early, turn, 0)

    loaded("yf")
    take(zrecv.at[pl.ds(0, cols - 1)], z_rs)

    x = jnp.concatenate([zrecv[s] for s in range(cols)], 1)
    depth = width_in * rk
    halves = stacked(x)
    both = dot(halves, yf_ref[0])
    y = both[:depth] + both[depth:] + dot(x.astype(BF16), yf_ref[1])
    lanes = yf_ref.shape[2] // 2
    wide = ypad.shape[1]
    parts = lanes // wide
    slot = ypad.shape[0] // parts
    ypad[...] = jnp.zeros_like(ypad)
    low_rows = iota((rk, lanes), 0) < rk // 2
    for j in range(width_in):
        here = y[j * rk:(j + 1) * rk]
        turned = pltpu.roll(here[:, lanes:], rk // 2, 0)
        here = here[:, :lanes] + jnp.where(low_rows, turned, -turned)
        for p in range(parts):
            ypad[p * slot + j * rk:p * slot + (j + 1) * rk, :] = here[:, p * wide:(p + 1) * wide]
    ysend[...] = jnp.transpose(ypad[...]).reshape(ysend.shape)
    for peer in row_peers:
        send(ysend.at[peer], yrecv.at[my_row], send_sems.at[1], y_rs, row=peer)
    yrecv[pl.ds(my_row, 1)] = ysend[pl.ds(my_row, 1)]

    lax.fori_loop(early, 2 * (KX // 8), turn, 0)
    loaded("tab", "ye")
    take(yrecv.at[pl.ds(0, rows - 1)], y_rs)

    a = xsend.shape[3]
    deep = yrecv.shape[1] // a
    is_re = (iota((rows * a, LANES), 1) % rk) < rk // 2
    plain, cross = [], []
    for l in range(deep):
        u = yrecv[:, l * a:(l + 1) * a, :].reshape(rows * a, LANES)
        plain.append(u)
        cross.append(jnp.where(is_re, pltpu.roll(u, LANES - rk // 2, 1), -pltpu.roll(u, rk // 2, 1)))
    u = jnp.concatenate([jnp.concatenate(plain, 1), jnp.concatenate(cross, 1)], 0)
    high, low = split(u)
    xf = tab_ref[at_xf:at_xf + 2 * KX, :2 * rows * a]
    both = dot(xf, high)
    q = both[:KX] + both[KX:] + dot(xf[:KX], low)
    halves = stacked(q)
    for j in range(width_in):
        both = dot(halves, tab_ref[at_sel + j * deep * LANES:at_sel + (j + 1) * deep * LANES, :])
        amp_ref[:, 2 * j * LANES:(2 * j + 2) * LANES] = both[:KX] + both[KX:]
    origin = jnp.where((my_row == 0) & (my_col == 0), 1.0, 0.0)
    flag = jnp.where((iota((KX, LANES), 0) == 0) & (iota((KX, LANES), 1) < oc), origin, 0.0)

    xb = tab_ref[at_xb:at_xb + rows * 2 * a, :6 * KX]

    def mix(c):
        pr = wt_ref[0, c * group + width_in] * flag
        pi = wt_ref[1, c * group + width_in] * flag
        for j in range(width_in):
            wr, wi = wt_ref[0, c * group + j], wt_ref[1, c * group + j]
            ar = amp_ref[:, (2 * j) * LANES:(2 * j + 1) * LANES]
            ai = amp_ref[:, (2 * j + 1) * LANES:(2 * j + 2) * LANES]
            pr = pr + (wr * ar - wi * ai)
            pi = pi + (wr * ai + wi * ar)
        high, low = split(jnp.concatenate([pr, pi], 0))
        xsend[c] = dot(xb, jnp.concatenate([high, low, high], 0)).reshape(xsend.shape[1:])
        for peer in row_peers:
            send(xsend.at[c, peer], xrecv.at[c, my_row], send_sems.at[2], x_rs.at[c], row=peer)
        xrecv[c, pl.ds(my_row, 1)] = xsend[c, pl.ds(my_row, 1)]

    tz = tab_ref[0:6 * KZ, :]
    side = rows * a
    middle = cells // 2
    upper = iota((ko, LANES), 1) >= LANES // 2

    def swap(first, second):
        return (
            jnp.where(upper, pltpu.roll(second, LANES // 2, 1), first),
            jnp.where(upper, second, pltpu.roll(first, LANES // 2, 1)),
        )

    def landing(c):
        return dlast_ref if c == chunks - 1 else crecv.at[c]

    def inverse_y(c):
        take(xrecv.at[c, pl.ds(0, rows - 1)], x_rs.at[c])
        turned = jnp.concatenate([xrecv[c, :, h].reshape(side, LANES) for h in range(2)], 0)
        turned = jnp.transpose(turned)
        held = [turned[l * ko:(l + 1) * ko] for l in range(kyl)]
        if side == LANES:
            held = [jnp.concatenate([x[:, h * side:(h + 1) * side] for x in held], 1) for h in range(2)]
        else:
            tiles = [swap(held[l], held[l + 1]) for l in range(0, kyl, 2)]
            held = [jnp.concatenate([x[h] for x in tiles], 1) for h in range(2)]
        halves = stacked(jnp.concatenate(held, 0))
        at = pl.ds(pl.multiple_of(my_col * 2 * ko, 2 * ko), 2 * ko)
        for i in range(0, cols, 2):
            targets = [lax.rem(my_col + i + 1, cols), lax.rem(my_col + i + 2, cols)]
            both = dot(halves, jnp.concatenate([ye_ref[d, 0] for d in targets], 1))
            acc = both[:2 * ko] + both[2 * ko:]
            acc = acc + dot(halves[:2 * ko], jnp.concatenate([ye_ref[d, 1] for d in targets], 1))
            for n, d in enumerate(targets):
                here = acc[:, n * LANES:(n + 1) * LANES]
                here = jnp.concatenate(swap(here[:ko], here[ko:]), 0)
                if i + n == cols - 1:
                    landing(c)[at, :] = here
                else:
                    csend[c, i + n] = here
                    send(csend.at[c, i + n], landing(c).at[at, :], send_sems.at[3], c_rs.at[c], col=d)

    def arrive(c):
        take(landing(c).at[pl.ds(0, (cols - 1) * 2 * ko), :], c_rs.at[c])

    def inverse_z(c):
        arrive(c)
        for i in range(oc):
            o = c * oc + i
            row = lambda j: comb_ref[o:o + 1, j * LANES:(j + 1) * LANES]
            d = crecv[c, pl.ds(i, cols * 2 * kzl, stride=oc), :]
            feats_ref[o] = one_channel(d, row, adv_ref, tz)

    mixed = 0
    for c in range(chunks):
        upto = min(ahead[min(c, len(ahead) - 1)], chunks)
        for n in range(mixed, upto):
            mix(n)
        mixed = max(mixed, upto)
        inverse_y(c)
        if 0 <= c - lag < chunks - 1:
            inverse_z(c - lag)
    for c in range(max(chunks - lag, 0), chunks - 1):
        inverse_z(c)
    arrive(chunks - 1)
    take(zsend.at[pl.ds(0, cols - 1)], send_sems.at[0])
    take(ysend.at[pl.ds(0, rows - 1)], send_sems.at[1])
    take(xsend.at[:, pl.ds(0, rows - 1)], send_sems.at[2])
    take(csend, send_sems.at[3])


def finish_kernel(oc, depth, *refs):
    if len(refs) == 8:
        feats_ref, refs = refs[0], refs[1:]
        first = feats_ref.shape[0]
    else:
        feats_ref, first = None, 0
    d_ref, adv_ref, comb_ref, tz_ref, out_ref, last_ref, sems = refs
    copies = []
    if feats_ref is not None:
        copies.append(pltpu.make_async_copy(feats_ref, out_ref.at[pl.ds(0, first)], sems.at[oc]))
        copies[0].start()
    for i in range(oc):
        o = first + i
        row = lambda j: comb_ref[o:o + 1, j * LANES:(j + 1) * LANES]
        last_ref[i] = one_channel(d_ref[pl.ds(i, depth, stride=oc), :], row, adv_ref, tz_ref[...])
        copy = pltpu.make_async_copy(last_ref.at[pl.ds(i, 1)], out_ref.at[pl.ds(o, 1)], sems.at[i])
        copy.start()
        copies.append(copy)
    for copy in copies:
        copy.wait()


def per_device(
    velocity, tendency, step_size, lift_weight, lift_bias, spectral_weight, local_weight, local_bias
):
    samples, width_in, a, b, nz = velocity.shape
    channels = lift_weight.shape[0]
    rows, cols = lax.axis_size("row"), lax.axis_size("col")
    full_x, full_y = a * rows, b * cols
    kzl, kyl = KZ // cols, KY // rows
    slots = kyl * kzl
    modes = slots * KX
    cells = a * b
    group = width_in + 1
    oc = LANES // slots
    chunks = channels // oc
    ko = kzl * oc
    lag, ahead = 5, (4, 5, 6, 7, 8)
    vmem = pl.BlockSpec(memory_space=pltpu.VMEM)
    anywhere = pl.BlockSpec(memory_space=pl.ANY)
    stored = spectral_weight.reshape(2 * modes, channels * channels)

    zc, zs = trig(np.arange(KZ), nz)
    rk = 2 * max(kzl, 4)
    zf = np.zeros((cols, 2, rk // 2, nz), np.float32)
    zf[:, :, :kzl] = np.stack([zc, -zs], 0).reshape(2, cols, kzl, nz).transpose(1, 0, 2, 3)
    zf2 = np.concatenate(np_halves(zf.reshape(cols * rk, nz)), 0)
    yc, ys = trig(waves(KY), full_y)
    xc, xs = trig(waves(KX), full_x)
    scale = 1.0 / (full_x * full_y * nz)
    xf2 = np.concatenate(np_halves(np.concatenate([xc, xs], 1) * scale), 0)
    parts = 2
    deep = kyl // parts
    slot = LANES // parts
    yf = np.stack([yc, ys], 0).reshape(2, rows, deep, parts, 1, cols, 1, b)
    yf = yf * np.eye(a).reshape(1, 1, 1, 1, a, 1, a, 1)
    yf = yf.transpose(0, 3, 1, 2, 4, 5, 6, 7).reshape(2 * parts * rows * deep * a, cols * cells).T
    yf = np.stack(np_halves(yf), 0)
    sel = np.zeros((deep, parts, slot, width_in, 2, kyl, kzl, oc), np.float32)
    for l in range(kyl):
        for j in range(width_in):
            for ri in range(2):
                for k in range(kzl):
                    sel[l // parts, l % parts, j * rk + ri * (rk // 2) + k, j, ri, l, k] = 1
    sel = sel.reshape(deep * LANES, width_in * 2 * LANES)
    xb = np.stack([np.stack([xc, -xs], 0), np.stack([xs, xc], 0)], 0)
    xb = xb.reshape(2, 2, KX, rows, 2, a // 2).transpose(3, 4, 0, 5, 1, 2).reshape(rows * 2 * a, 2 * KX)
    xbh, xbl = np_halves(xb)
    xb3 = np.concatenate([xbh, xbh, xbl], 1)
    yb = np.stack([np.stack([yc, ys], 0), np.stack([-ys, yc], 0)], 0)
    yb = yb.reshape(2, 2, rows, kyl, cols, b).transpose(4, 3, 2, 0, 1, 5)
    yb = yb.reshape(cols, kyl, rows, 2, 1, 2, 1, b) * np.eye(a // 2).reshape(a // 2, 1, a // 2, 1)
    ye = np.stack(np_halves(yb.reshape(cols, kyl * rows * a, cells)), 1)
    twice = np.where(np.arange(KZ) == 0, 1.0, 2.0)[:, None]
    zb = np.stack([twice * zc, -twice * zs], 0).reshape(2, cols, kzl, nz).transpose(1, 0, 2, 3).reshape(2 * KZ, nz)
    zbh, zbl = np_halves(zb)
    zb3 = np.concatenate([zbh, zbh, zbl], 0)
    tz = jnp.asarray(zb3)
    sel = sel.reshape(deep * LANES, width_in, 2 * LANES).transpose(1, 0, 2).reshape(-1, 2 * LANES)
    pieces = [zb3, xf2, sel, xb3]
    table = np.concatenate([np.pad(np.asarray(x, jnp.bfloat16), ((0, 0), (0, nz - x.shape[1]))) for x in pieces], 0)
    starts = [zb3.shape[0], zb3.shape[0] + xf2.shape[0], zb3.shape[0] + xf2.shape[0] + sel.shape[0]]

    results = []
    for sample in range(samples):
        inputs = [
            velocity[sample].reshape(width_in, cells, nz), tendency[sample].reshape(width_in, cells, nz),
            step_size[sample].reshape(1, 1), lift_weight.T, lift_bias.reshape(1, channels), local_weight,
            local_bias.reshape(1, channels), jnp.asarray(zf2), jnp.asarray(yf), jnp.asarray(ye), jnp.asarray(table), stored,
        ]
        dma = lambda *shape: pltpu.SemaphoreType.DMA(shape)
        first = channels - oc
        outs = [
            jax.ShapeDtypeStruct((cols * 2 * ko, cells), F32),
            jax.ShapeDtypeStruct((width_in, cells, nz), F32),
            jax.ShapeDtypeStruct((channels, group * LANES), F32),
        ]
        if first:
            outs = [jax.ShapeDtypeStruct((first, cells, nz), BF16)] + outs
        held = pl.pallas_call(
            functools.partial(layer_kernel, kyl, kzl, oc, lag, ahead, *starts),
            out_shape=outs,
            in_specs=[anywhere] * len(inputs),
            out_specs=[vmem] * len(outs),
            scratch_shapes=[pltpu.VMEM(x.shape, x.dtype) for x in inputs] + [
                pltpu.VMEM((channels * channels, 2 * LANES), BF16),
                pltpu.VMEM((2 * modes, LANES), F32),
                pltpu.VMEM((2, slots, KX, LANES), F32),
                pltpu.VMEM((cols, width_in * rk, cells), F32),
                pltpu.VMEM((cols, width_in * rk, cells), F32),
                pltpu.VMEM((parts * slot, rows * deep * a), F32),
                pltpu.VMEM((rows, deep * a, LANES), F32),
                pltpu.VMEM((rows, deep * a, LANES), F32),
                pltpu.VMEM((KX, width_in * 2 * LANES), F32),
                pltpu.VMEM((chunks, rows, 2, a, LANES), F32),
                pltpu.VMEM((chunks, rows, 2, a, LANES), F32),
                pltpu.VMEM((chunks, cols - 1, 2 * ko, cells), F32),
                pltpu.VMEM((chunks, cols * 2 * ko, cells), F32),
                dma(len(inputs)), dma(4), pltpu.SemaphoreType.DMA, pltpu.SemaphoreType.DMA, dma(chunks), dma(chunks),
            ],
            compiler_params=pltpu.CompilerParams(
                vmem_limit_bytes=40 * 1024 * 1024, collective_id=0, has_side_effects=True
            ),
        )(*[x if x.size == 1 else pltpu.with_memory_space_constraint(x, pltpu.HBM) for x in inputs])
        features = pl.pallas_call(
            functools.partial(finish_kernel, oc, cols * 2 * kzl),
            out_shape=jax.ShapeDtypeStruct((channels, cells, nz), BF16),
            in_specs=[vmem] * (len(held) + 1),
            out_specs=anywhere,
            scratch_shapes=[pltpu.VMEM((oc, cells, nz), BF16), dma(oc + 1)],
            compiler_params=pltpu.CompilerParams(vmem_limit_bytes=16 * 1024 * 1024),
        )(*held, tz)
        results.append(features.reshape(channels, a, b, nz))
    return jnp.stack(results, 0)


def solution(mesh):
    in_specs = (
        P(None, None, "row", "col", None),
        P(None, None, "row", "col", None),
        P(),
        P(),
        P(),
        P(None, "row", "col", None, None),
        P(),
        P(),
    )
    out_specs = P(None, None, "row", "col", None)
    return jax.shard_map(
        per_device, mesh=mesh, in_specs=in_specs, out_specs=out_specs, check_vma=False
    )
```

```python
import functools
import math

import jax
import jax.numpy as jnp
import numpy as np
from jax import lax
from jax.experimental import pallas as pl
from jax.experimental.pallas import tpu as pltpu
from jax.sharding import PartitionSpec as P

KX = 32
KY = 32
KZ = 32
LANES = 128
HIGHEST = lax.Precision.HIGHEST
F32 = jnp.float32
BF16 = jnp.bfloat16
MESH = pl.DeviceIdType.MESH


def waves(count):
    index = np.arange(count)
    return np.where(index < count // 2, index, index - count)


def trig(wave, length):
    angle = ((wave[:, None] * np.arange(length)[None, :]) % length) * (2.0 * math.pi / length)
    return np.cos(angle), np.sin(angle)


def np_halves(table):
    table = np.asarray(table, np.float32)
    high = table.astype(jnp.bfloat16)
    low = (table - high.astype(np.float32)).astype(jnp.bfloat16)
    return high, low


def split(x):
    high = x.astype(BF16)
    return high, (x - high.astype(F32)).astype(BF16)


def stacked(x):
    high = x.astype(BF16).astype(F32)
    return jnp.concatenate([high, x - high], 0).astype(BF16)


def dot(a, b):
    return jnp.dot(a, b, preferred_element_type=F32)


def dot_rows(a, b, precision=None):
    return lax.dot_general(a, b, (((0,), (0,)), ((), ())), precision=precision, preferred_element_type=F32)


def dot_lanes(a, b):
    return lax.dot_general(a, b, (((1,), (1,)), ((), ())), preferred_element_type=F32)


def iota(shape, axis):
    return lax.broadcasted_iota(jnp.int32, shape, axis)


def one_channel(d, row, adv_ref, tz):
    width_in = adv_ref.shape[0]
    d = d + jnp.where(iota(d.shape, 0) == 0, row(width_in), 0.0)
    high, low = split(d)
    x = dot_rows(jnp.concatenate([high, low, high], 0), tz)
    for j in range(width_in):
        weight = row(j)
        x = x + jnp.concatenate([weight] * (x.shape[1] // LANES), 1) * adv_ref[j]
    inner = x * (0.7978845608028654 + 0.035677408136300125 * (x * x))
    half = 0.5 * x
    return (half + half * jnp.tanh(inner)).astype(BF16)


def layer_kernel(
    kyl, kzl, oc, lag, ahead, at_xf, at_sel, at_xb, vel_any, tend_any, step_any, lw_any, lb_any, cw_any, cb_any, zf_any,
    yf_any, ye_any, tab_any, w_any, *rest,
):
    chunks = LANES // (oc * (lw_any.shape[0] + 1))
    if chunks > 1:
        feats_ref, rest = rest[0], rest[1:]
    else:
        feats_ref = None
    (
        dlast_ref, adv_ref, comb_ref, vel_ref, tend_ref, step_ref, lw_ref, lb_ref, cw_ref, cb_ref, zf_ref, yf_ref, ye_ref,
        tab_ref, w_ref, lift_ref, wl_ref, wt_ref, zsend, zrecv, ypad, ysend, yrecv, amp_ref, xsend, xrecv, csend, crecv,
        in_sems, send_sems, z_rs, y_rs, x_rs, c_rs,
    ) = rest
    rows, cols = lax.axis_size("row"), lax.axis_size("col")
    my_row, my_col = lax.axis_index("row"), lax.axis_index("col")
    width_in, cells, _ = vel_ref.shape
    channels = cw_ref.shape[0]
    group = width_in + 1
    freq = zf_ref.shape[0] // 2
    rk = freq // cols
    slots = kyl * kzl
    modes = slots * KX
    ko = kzl * oc
    early = 4

    barrier = pltpu.get_barrier_semaphore()
    row_peers = [lax.rem(my_row + i, rows) for i in range(1, rows)]
    col_peers = [lax.rem(my_col + i, cols) for i in range(1, cols)]
    def greet():
      for peer in row_peers:
          pl.semaphore_signal(barrier, inc=1, device_id={"row": peer}, device_id_type=MESH)
      for peer in col_peers:
          pl.semaphore_signal(barrier, inc=1, device_id={"col": peer}, device_id_type=MESH)

    loads = {}
    order = [
        ("vel", vel_any, vel_ref), ("tend", tend_any, tend_ref), ("step", step_any, step_ref), ("zf", zf_any, zf_ref),
        ("lw", lw_any, lw_ref), ("lb", lb_any, lb_ref), ("cw", cw_any, cw_ref), ("cb", cb_any, cb_ref),
        ("w", w_any, w_ref), ("yf", yf_any, yf_ref), ("tab", tab_any, tab_ref), ("ye", ye_any, ye_ref),
    ]
    for n, (name, source, target) in enumerate(order):
        loads[name] = pltpu.make_async_copy(source, target, in_sems.at[n])
        loads[name].start()
        if name == "step":
            greet()

    def loaded(*names):
        for name in names:
            loads[name].wait()

    def send(source, target, sends, receives, **where):
        pltpu.make_async_remote_copy(source, target, sends, receives, device_id=where, device_id_type=MESH).start()

    def take(ref, semaphore):
        pltpu.make_async_copy(ref, ref, semaphore).wait()

    def send_z(j):
        at = pl.ds(j * rk, rk)
        for peer in col_peers:
            send(zsend.at[peer, at], zrecv.at[my_col, at], send_sems.at[0], z_rs, col=peer)

    loaded("vel", "tend", "step", "zf")
    step = step_ref[0:1, 0:1]
    for j in range(width_in):
        adv = vel_ref[j] + step * tend_ref[j]
        adv_ref[j] = adv
        high, low = split(adv)
        both = dot_lanes(zf_ref[...], high)
        z = both[:freq] + both[freq:] + dot_lanes(zf_ref[0:freq, :], low)
        zsend[:, j * rk:(j + 1) * rk, :] = z.reshape(cols, rk, cells)
        if j == 0:
            pl.semaphore_wait(barrier, rows + cols - 2)
        send_z(j)
    zrecv[pl.ds(my_col, 1)] = zsend[pl.ds(my_col, 1)]

    loaded("lw", "lb", "cw", "cb")
    eight = iota((8, channels), 0)
    lift = jnp.where(eight == width_in, lb_ref[...], 0.0)
    for j in range(width_in):
        lift = jnp.where(eight == j, lw_ref[j:j + 1, :], lift)
    block = iota((8, LANES), 1) // oc
    pick = jnp.where(block % group == iota((8, LANES), 0), 1.0, 0.0)
    spread = dot_rows(lift, pick, HIGHEST)
    high = spread.astype(BF16).astype(F32)
    low = spread - high
    lane = iota((channels, LANES), 1)
    owner = (lane // (oc * group)) * oc + lane % oc
    for o in range(channels):
        at = slice(o * channels, (o + 1) * channels)
        lift_ref[at, :LANES] = jnp.where(owner == o, high, 0.0).astype(BF16)
        lift_ref[at, LANES:] = jnp.where(owner == o, low, 0.0).astype(BF16)
    wide = (8, group * LANES)
    spread = dot_rows(lift, jnp.where(iota(wide, 1) // LANES == iota(wide, 0), 1.0, 0.0), HIGHEST)
    comb = jnp.dot(cw_ref[...], spread, precision=HIGHEST, preferred_element_type=F32)
    bias = jnp.where(eight == 0, cb_ref[...], 0.0)
    bias = dot_rows(bias, jnp.where(iota((8, LANES), 0) == 0, 1.0, 0.0), HIGHEST)
    comb_ref[:, :width_in * LANES] = comb[:, :width_in * LANES]
    comb_ref[:, width_in * LANES:] = comb[:, width_in * LANES:] + bias

    loaded("w")
    step_rows = modes // 2

    def weigh(n):
        at = slice(n * step_rows, (n + 1) * step_rows)
        both = dot(w_ref[at, :], lift_ref[...])
        wl_ref[at, :] = both[:, :LANES] + both[:, LANES:]

    for n in range(4):
        weigh(n)

    def turn(n, carry):
        ri, at = n // (KX // 8), (n % (KX // 8)) * 8
        held = [wl_ref[pl.ds(pl.multiple_of(ri * modes + s * KX + at, 8), 8), :] for s in range(slots)]
        held = [pltpu.roll(x, s * oc, 1) if s else x for s, x in enumerate(held)]
        held = [held[-s % slots] for s in range(slots)]
        place = iota((8, LANES), 1) // oc
        bit = 1
        while bit < slots:
            upper = (place // bit) % 2 == 1
            held = [jnp.where(upper, held[(s - bit) % slots], held[s]) for s in range(slots)]
            bit *= 2
        held = [pltpu.roll(x, LANES - s * oc, 1) if s else x for s, x in enumerate(held)]
        for s in range(slots):
            wt_ref[ri, s, pl.ds(pl.multiple_of(at, 8), 8), :] = held[s]
        return carry

    lax.fori_loop(0, early, turn, 0)

    loaded("yf")
    take(zrecv.at[pl.ds(0, cols - 1)], z_rs)

    x = jnp.concatenate([zrecv[s] for s in range(cols)], 1)
    depth = width_in * rk
    halves = stacked(x)
    both = dot(halves, yf_ref[0])
    y = both[:depth] + both[depth:] + dot(x.astype(BF16), yf_ref[1])
    lanes = yf_ref.shape[2] // 2
    wide = ypad.shape[1]
    parts = lanes // wide
    slot = ypad.shape[0] // parts
    ypad[...] = jnp.zeros_like(ypad)
    low_rows = iota((rk, lanes), 0) < rk // 2
    for j in range(width_in):
        here = y[j * rk:(j + 1) * rk]
        turned = pltpu.roll(here[:, lanes:], rk // 2, 0)
        here = here[:, :lanes] + jnp.where(low_rows, turned, -turned)
        for p in range(parts):
            ypad[p * slot + j * rk:p * slot + (j + 1) * rk, :] = here[:, p * wide:(p + 1) * wide]
    ysend[...] = jnp.transpose(ypad[...]).reshape(ysend.shape)
    for peer in row_peers:
        send(ysend.at[peer], yrecv.at[my_row], send_sems.at[1], y_rs, row=peer)
    yrecv[pl.ds(my_row, 1)] = ysend[pl.ds(my_row, 1)]

    lax.fori_loop(early, 2 * (KX // 8), turn, 0)
    loaded("tab", "ye")
    take(yrecv.at[pl.ds(0, rows - 1)], y_rs)

    a = xsend.shape[3]
    deep = yrecv.shape[1] // a
    is_re = (iota((rows * a, LANES), 1) % rk) < rk // 2
    plain, cross = [], []
    for l in range(deep):
        u = yrecv[:, l * a:(l + 1) * a, :].reshape(rows * a, LANES)
        plain.append(u)
        cross.append(jnp.where(is_re, pltpu.roll(u, LANES - rk // 2, 1), -pltpu.roll(u, rk // 2, 1)))
    u = jnp.concatenate([jnp.concatenate(plain, 1), jnp.concatenate(cross, 1)], 0)
    high, low = split(u)
    xf = tab_ref[at_xf:at_xf + 2 * KX, :2 * rows * a]
    both = dot(xf, high)
    q = both[:KX] + both[KX:] + dot(xf[:KX], low)
    halves = stacked(q)
    for j in range(width_in):
        both = dot(halves, tab_ref[at_sel + j * deep * LANES:at_sel + (j + 1) * deep * LANES, :])
        amp_ref[:, 2 * j * LANES:(2 * j + 2) * LANES] = both[:KX] + both[KX:]
    origin = jnp.where((my_row == 0) & (my_col == 0), 1.0, 0.0)
    flag = jnp.where((iota((KX, LANES), 0) == 0) & (iota((KX, LANES), 1) < oc), origin, 0.0)

    xb = tab_ref[at_xb:at_xb + rows * 2 * a, :6 * KX]

    def mix(c):
        pr = wt_ref[0, c * group + width_in] * flag
        pi = wt_ref[1, c * group + width_in] * flag
        for j in range(width_in):
            wr, wi = wt_ref[0, c * group + j], wt_ref[1, c * group + j]
            ar = amp_ref[:, (2 * j) * LANES:(2 * j + 1) * LANES]
            ai = amp_ref[:, (2 * j + 1) * LANES:(2 * j + 2) * LANES]
            pr = pr + (wr * ar - wi * ai)
            pi = pi + (wr * ai + wi * ar)
        high, low = split(jnp.concatenate([pr, pi], 0))
        xsend[c] = dot(xb, jnp.concatenate([high, low, high], 0)).reshape(xsend.shape[1:])
        for peer in row_peers:
            send(xsend.at[c, peer], xrecv.at[c, my_row], send_sems.at[2], x_rs.at[c], row=peer)
        xrecv[c, pl.ds(my_row, 1)] = xsend[c, pl.ds(my_row, 1)]

    tz = tab_ref[0:6 * KZ, :]
    side = rows * a
    middle = cells // 2
    upper = iota((ko, LANES), 1) >= LANES // 2

    def swap(first, second):
        return (
            jnp.where(upper, pltpu.roll(second, LANES // 2, 1), first),
            jnp.where(upper, second, pltpu.roll(first, LANES // 2, 1)),
        )

    def landing(c):
        return dlast_ref if c == chunks - 1 else crecv.at[c]

    def inverse_y(c):
        take(xrecv.at[c, pl.ds(0, rows - 1)], x_rs.at[c])
        turned = jnp.concatenate([xrecv[c, :, h].reshape(side, LANES) for h in range(2)], 0)
        turned = jnp.transpose(turned)
        held = [turned[l * ko:(l + 1) * ko] for l in range(kyl)]
        if side == LANES:
            held = [jnp.concatenate([x[:, h * side:(h + 1) * side] for x in held], 1) for h in range(2)]
        else:
            tiles = [swap(held[l], held[l + 1]) for l in range(0, kyl, 2)]
            held = [jnp.concatenate([x[h] for x in tiles], 1) for h in range(2)]
        halves = stacked(jnp.concatenate(held, 0))
        at = pl.ds(pl.multiple_of(my_col * 2 * ko, 2 * ko), 2 * ko)
        for i in range(0, cols, 2):
            targets = [lax.rem(my_col + i + 1, cols), lax.rem(my_col + i + 2, cols)]
            both = dot(halves, jnp.concatenate([ye_ref[d, 0] for d in targets], 1))
            acc = both[:2 * ko] + both[2 * ko:]
            acc = acc + dot(halves[:2 * ko], jnp.concatenate([ye_ref[d, 1] for d in targets], 1))
            for n, d in enumerate(targets):
                here = acc[:, n * LANES:(n + 1) * LANES]
                here = jnp.concatenate(swap(here[:ko], here[ko:]), 0)
                if i + n == cols - 1:
                    landing(c)[at, :] = here
                else:
                    csend[c, i + n] = here
                    send(csend.at[c, i + n], landing(c).at[at, :], send_sems.at[3], c_rs.at[c], col=d)

    def arrive(c):
        take(landing(c).at[pl.ds(0, (cols - 1) * 2 * ko), :], c_rs.at[c])

    def inverse_z(c):
        arrive(c)
        for i in range(oc):
            o = c * oc + i
            row = lambda j: comb_ref[o:o + 1, j * LANES:(j + 1) * LANES]
            d = crecv[c, pl.ds(i, cols * 2 * kzl, stride=oc), :]
            feats_ref[o] = one_channel(d, row, adv_ref, tz)

    mixed = 0
    for c in range(chunks):
        upto = min(ahead[min(c, len(ahead) - 1)], chunks)
        for n in range(mixed, upto):
            mix(n)
        mixed = max(mixed, upto)
        inverse_y(c)
        if 0 <= c - lag < chunks - 1:
            inverse_z(c - lag)
    for c in range(max(chunks - lag, 0), chunks - 1):
        inverse_z(c)
    arrive(chunks - 1)
    take(zsend.at[pl.ds(0, cols - 1)], send_sems.at[0])
    take(ysend.at[pl.ds(0, rows - 1)], send_sems.at[1])
    take(xsend.at[:, pl.ds(0, rows - 1)], send_sems.at[2])
    take(csend, send_sems.at[3])


def finish_kernel(oc, depth, *refs):
    if len(refs) == 8:
        feats_ref, refs = refs[0], refs[1:]
        first = feats_ref.shape[0]
    else:
        feats_ref, first = None, 0
    d_ref, adv_ref, comb_ref, tz_ref, out_ref, last_ref, sems = refs
    copies = []
    if feats_ref is not None:
        copies.append(pltpu.make_async_copy(feats_ref, out_ref.at[pl.ds(0, first)], sems.at[oc]))
        copies[0].start()
    for i in range(oc):
        o = first + i
        row = lambda j: comb_ref[o:o + 1, j * LANES:(j + 1) * LANES]
        last_ref[i] = one_channel(d_ref[pl.ds(i, depth, stride=oc), :], row, adv_ref, tz_ref[...])
        copy = pltpu.make_async_copy(last_ref.at[pl.ds(i, 1)], out_ref.at[pl.ds(o, 1)], sems.at[i])
        copy.start()
        copies.append(copy)
    for copy in copies:
        copy.wait()


def per_device(
    velocity, tendency, step_size, lift_weight, lift_bias, spectral_weight, local_weight, local_bias
):
    samples, width_in, a, b, nz = velocity.shape
    channels = lift_weight.shape[0]
    rows, cols = lax.axis_size("row"), lax.axis_size("col")
    full_x, full_y = a * rows, b * cols
    kzl, kyl = KZ // cols, KY // rows
    slots = kyl * kzl
    modes = slots * KX
    cells = a * b
    group = width_in + 1
    oc = LANES // slots
    chunks = channels // oc
    ko = kzl * oc
    lag, ahead = 5, (4, 5, 6, 7, 8)
    vmem = pl.BlockSpec(memory_space=pltpu.VMEM)
    anywhere = pl.BlockSpec(memory_space=pl.ANY)
    stored = spectral_weight.reshape(2 * modes, channels * channels)

    zc, zs = trig(np.arange(KZ), nz)
    rk = 2 * max(kzl, 4)
    zf = np.zeros((cols, 2, rk // 2, nz), np.float32)
    zf[:, :, :kzl] = np.stack([zc, -zs], 0).reshape(2, cols, kzl, nz).transpose(1, 0, 2, 3)
    zf2 = np.concatenate(np_halves(zf.reshape(cols * rk, nz)), 0)
    yc, ys = trig(waves(KY), full_y)
    xc, xs = trig(waves(KX), full_x)
    scale = 1.0 / (full_x * full_y * nz)
    xf2 = np.concatenate(np_halves(np.concatenate([xc, xs], 1) * scale), 0)
    parts = 2
    deep = kyl // parts
    slot = LANES // parts
    yf = np.stack([yc, ys], 0).reshape(2, rows, deep, parts, 1, cols, 1, b)
    yf = yf * np.eye(a).reshape(1, 1, 1, 1, a, 1, a, 1)
    yf = yf.transpose(0, 3, 1, 2, 4, 5, 6, 7).reshape(2 * parts * rows * deep * a, cols * cells).T
    yf = np.stack(np_halves(yf), 0)
    sel = np.zeros((deep, parts, slot, width_in, 2, kyl, kzl, oc), np.float32)
    for l in range(kyl):
        for j in range(width_in):
            for ri in range(2):
                for k in range(kzl):
                    sel[l // parts, l % parts, j * rk + ri * (rk // 2) + k, j, ri, l, k] = 1
    sel = sel.reshape(deep * LANES, width_in * 2 * LANES)
    xb = np.stack([np.stack([xc, -xs], 0), np.stack([xs, xc], 0)], 0)
    xb = xb.reshape(2, 2, KX, rows, 2, a // 2).transpose(3, 4, 0, 5, 1, 2).reshape(rows * 2 * a, 2 * KX)
    xbh, xbl = np_halves(xb)
    xb3 = np.concatenate([xbh, xbh, xbl], 1)
    yb = np.stack([np.stack([yc, ys], 0), np.stack([-ys, yc], 0)], 0)
    yb = yb.reshape(2, 2, rows, kyl, cols, b).transpose(4, 3, 2, 0, 1, 5)
    yb = yb.reshape(cols, kyl, rows, 2, 1, 2, 1, b) * np.eye(a // 2).reshape(a // 2, 1, a // 2, 1)
    ye = np.stack(np_halves(yb.reshape(cols, kyl * rows * a, cells)), 1)
    twice = np.where(np.arange(KZ) == 0, 1.0, 2.0)[:, None]
    zb = np.stack([twice * zc, -twice * zs], 0).reshape(2, cols, kzl, nz).transpose(1, 0, 2, 3).reshape(2 * KZ, nz)
    zbh, zbl = np_halves(zb)
    zb3 = np.concatenate([zbh, zbh, zbl], 0)
    tz = jnp.asarray(zb3)
    sel = sel.reshape(deep * LANES, width_in, 2 * LANES).transpose(1, 0, 2).reshape(-1, 2 * LANES)
    pieces = [zb3, xf2, sel, xb3]
    table = np.concatenate([np.pad(np.asarray(x, jnp.bfloat16), ((0, 0), (0, nz - x.shape[1]))) for x in pieces], 0)
    starts = [zb3.shape[0], zb3.shape[0] + xf2.shape[0], zb3.shape[0] + xf2.shape[0] + sel.shape[0]]

    results = []
    for sample in range(samples):
        inputs = [
            velocity[sample].reshape(width_in, cells, nz), tendency[sample].reshape(width_in, cells, nz),
            step_size[sample].reshape(1, 1), lift_weight.T, lift_bias.reshape(1, channels), local_weight,
            local_bias.reshape(1, channels), jnp.asarray(zf2), jnp.asarray(yf), jnp.asarray(ye), jnp.asarray(table), stored,
        ]
        dma = lambda *shape: pltpu.SemaphoreType.DMA(shape)
        first = channels - oc
        outs = [
            jax.ShapeDtypeStruct((cols * 2 * ko, cells), F32),
            jax.ShapeDtypeStruct((width_in, cells, nz), F32),
            jax.ShapeDtypeStruct((channels, group * LANES), F32),
        ]
        if first:
            outs = [jax.ShapeDtypeStruct((first, cells, nz), BF16)] + outs
        held = pl.pallas_call(
            functools.partial(layer_kernel, kyl, kzl, oc, lag, ahead, *starts),
            out_shape=outs,
            in_specs=[anywhere] * len(inputs),
            out_specs=[vmem] * len(outs),
            scratch_shapes=[pltpu.VMEM(x.shape, x.dtype) for x in inputs] + [
                pltpu.VMEM((channels * channels, 2 * LANES), BF16),
                pltpu.VMEM((2 * modes, LANES), F32),
                pltpu.VMEM((2, slots, KX, LANES), F32),
                pltpu.VMEM((cols, width_in * rk, cells), F32),
                pltpu.VMEM((cols, width_in * rk, cells), F32),
                pltpu.VMEM((parts * slot, rows * deep * a), F32),
                pltpu.VMEM((rows, deep * a, LANES), F32),
                pltpu.VMEM((rows, deep * a, LANES), F32),
                pltpu.VMEM((KX, width_in * 2 * LANES), F32),
                pltpu.VMEM((chunks, rows, 2, a, LANES), F32),
                pltpu.VMEM((chunks, rows, 2, a, LANES), F32),
                pltpu.VMEM((chunks, cols - 1, 2 * ko, cells), F32),
                pltpu.VMEM((chunks, cols * 2 * ko, cells), F32),
                dma(len(inputs)), dma(4), pltpu.SemaphoreType.DMA, pltpu.SemaphoreType.DMA, dma(chunks), dma(chunks),
            ],
            compiler_params=pltpu.CompilerParams(
                vmem_limit_bytes=40 * 1024 * 1024, collective_id=0, has_side_effects=True
            ),
        )(*[x if x.size == 1 else pltpu.with_memory_space_constraint(x, pltpu.HBM) for x in inputs])
        features = pl.pallas_call(
            functools.partial(finish_kernel, oc, cols * 2 * kzl),
            out_shape=jax.ShapeDtypeStruct((channels, cells, nz), BF16),
            in_specs=[vmem] * (len(held) + 1),
            out_specs=anywhere,
            scratch_shapes=[pltpu.VMEM((oc, cells, nz), BF16), dma(oc + 1)],
            compiler_params=pltpu.CompilerParams(vmem_limit_bytes=16 * 1024 * 1024),
        )(*held, tz)
        results.append(features.reshape(channels, a, b, nz))
    return jnp.stack(results, 0)


def solution(mesh):
    in_specs = (
        P(None, None, "row", "col", None),
        P(None, None, "row", "col", None),
        P(),
        P(),
        P(),
        P(None, "row", "col", None, None),
        P(),
        P(),
    )
    out_specs = P(None, None, "row", "col", None)
    return jax.shard_map(
        per_device, mesh=mesh, in_specs=in_specs, out_specs=out_specs, check_vma=False
    )
```
